256 devices in a mesh: dp: 16 (over z, y_lo), mp: 16 (over y_hi, x, core).
Axes of the slice: x: 4, y: 4 (y_hi: 2, y_lo: 2; y = y_hi * 2 + y_lo), z: 8, core: 2. Of those that a mesh axis runs over, the one named last changes fastest.
Arguments:
- gradient: bfloat16 [1, 4096, 4096], P(None, 'mp', 'dp'), may hold values from -6 to 6
- first_moment: float32 [1, 4096, 4096], P(None, 'mp', 'dp'), may hold values from -3 to 3
- second_moment: float32 [1, 4096, 4096], P(None, 'mp', 'dp'), may hold values from 0.0625 to 1
- left_factor: float32 [1, 4096, 4096], P(None, 'mp', 'dp'), may hold values from -18 to 18
- right_factor: float32 [1, 4096, 4096], P(None, 'mp', 'dp'), may hold values from -18 to 18
- left_basis: bfloat16 [1, 4096, 4096], P(None, 'dp', 'mp'), may hold values from -0.09375 to 0.09375
- right_basis: bfloat16 [1, 4096, 4096], P(None, 'mp', 'dp'), may hold values from -0.09375 to 0.09375
Outputs:
- new_first_moment: float32 [1, 4096, 4096], P(None, 'mp', 'dp')
- new_second_moment: float32 [1, 4096, 4096], P(None, 'mp', 'dp')
- new_left_factor: float32 [1, 4096, 4096], P(None, 'mp', 'dp')
- new_right_factor: float32 [1, 4096, 4096], P(None, 'mp', 'dp')
- update: bfloat16 [1, 4096, 4096], P(None, 'mp', 'dp')
The draws below stay inside these ranges and needn't reach their ends.
All inputs are finite; a program needn't handle non-finite values.
Results may differ from the reference program's by a relative error of at most 0.014.
Values may be sent and summed in bfloat16 or wider, within the bound.
A program may use at most 64 MiB of HBM per device.

```python
import math
import jax
import jax.numpy as jnp
from jax import lax

B = 4096
BLOCKS = 1


def shard_levels(rng, dims, split, low, high):
    def one(position, shards_of):
        steps = jax.random.uniform(jax.random.fold_in(jax.random.fold_in(rng, 6), position), (shards_of,), jnp.float32, low / len(split), high / len(split))
        return jnp.repeat(jnp.exp(steps), dims[position] // shards_of).reshape((-1,) + (1,) * (len(dims) - position - 1))

    level = one(*split[0])
    for cut in split[1:]:
        level = level * one(*cut)
    return level


def scatter_about(stream_key, shape, spread, reach, split=(), dtype=jnp.bfloat16):
    drawn = spread * jax.random.normal(stream_key, shape, jnp.float32)
    if split:
        drawn = drawn * shard_levels(stream_key, shape, split, -0.22, 0.18)
    return jnp.clip(drawn, -reach, reach).astype(dtype)


def setup_inputs(seed: int = 0) -> dict:
    splits = jax.random.split(jax.random.key(seed), 8)
    gradient = scatter_about(splits[0], (BLOCKS, B, B), 1.0, 6.0, ((1, 16), (2, 16)))
    first_moment = scatter_about(splits[1], (BLOCKS, B, B), 0.5, 3.0, ((1, 16), (2, 16)), jnp.float32)
    second_moment = jnp.clip(jnp.exp(math.log(1.0) - 2.7725887 * jax.random.uniform(splits[2], (BLOCKS, B, B), jnp.float32) ** shard_levels(splits[2], (BLOCKS, B, B), ((1, 16), (2, 16)), -0.2, 0.2)), 0.0625, 1.0)
    left_factor = scatter_about(splits[3], (BLOCKS, B, B), 3.0, 18.0, ((1, 16), (2, 16)), jnp.float32)
    right_factor = scatter_about(splits[4], (BLOCKS, B, B), 3.0, 18.0, ((1, 16), (2, 16)), jnp.float32)
    left_basis = scatter_about(splits[5], (BLOCKS, B, B), B ** -0.5, 0.09375, ((1, 16), (2, 16)))
    right_basis = scatter_about(splits[6], (BLOCKS, B, B), B ** -0.5, 0.09375, ((1, 16), (2, 16)))
    return {"gradient": gradient, "first_moment": first_moment, "second_moment": second_moment, "left_factor": left_factor, "right_factor": right_factor, "left_basis": left_basis, "right_basis": right_basis}


decay_moment = 0.95
decay_factor = 0.95
epsilon = 1e-08

def product(left, right):
    return jnp.dot(left.astype(jnp.float32), right.astype(jnp.float32), precision=lax.Precision.HIGHEST)

def single_block(operands):
    gradient, first_moment, second_moment, left_factor, right_factor, left_basis, right_basis = operands
    scale = 1.0 - decay_factor
    new_left = decay_factor * left_factor + scale * product(gradient, gradient.T)
    new_right = decay_factor * right_factor + scale * product(gradient.T, gradient)
    rotated_left = product(left_basis.T, gradient).astype(jnp.bfloat16)
    rotated = product(rotated_left, right_basis)
    new_first = decay_moment * first_moment + (1.0 - decay_moment) * rotated
    new_second = decay_moment * second_moment + (1.0 - decay_moment) * rotated * rotated
    direction = (new_first / (jnp.sqrt(new_second) + epsilon)).astype(jnp.bfloat16)
    back_left = product(left_basis, direction).astype(jnp.bfloat16)
    update = product(back_left, right_basis.T).astype(jnp.bfloat16)
    return (new_first, new_second, new_left, new_right, update)

def reference(gradient, first_moment, second_moment, left_factor, right_factor, left_basis, right_basis):
    first_out, second_out, left_out, right_out, update_out = lax.map(single_block, (gradient, first_moment, second_moment, left_factor, right_factor, left_basis, right_basis))
    return (first_out, second_out, left_out, right_out, update_out)
```

```python
import jax
import jax.numpy as jnp
from jax import lax
from jax.experimental import pallas as pl
from jax.experimental.pallas import tpu as pltpu
from jax.sharding import PartitionSpec as P

decay_moment = 0.95
decay_factor = 0.95
epsilon = 1e-08
N = 256
H = N // 2
NZ = 8
NX = 4
NSEM = 400

BF = jnp.bfloat16
F32 = jnp.float32


def dot(a, b):
    return jnp.dot(a, b, preferred_element_type=F32)


def turned(a):
    return a.astype(F32).T


class Place:
    def __init__(self):
        self.j = lax.axis_index("dp")
        self.i = lax.axis_index("mp")
        self.z, self.yl = self.j // 2, self.j % 2
        self.yh, self.x, self.c = self.i // 8, (self.i // 2) % NX, self.i % 2

    def device(self, dz=0, dy=0, dh=0, dx=0, dc=0):
        return {"dp": self.dp(dz, dy), "mp": self.mp(dh, dx, dc)}

    def dp(self, dz=0, dy=0):
        yl = 1 - self.yl if dy else self.yl
        return lax.rem(self.z + dz + NZ, NZ) * 2 + yl

    def mp(self, dh=0, dx=0, dc=0):
        yh = 1 - self.yh if dh else self.yh
        c = 1 - self.c if dc else self.c
        return yh * 8 + lax.rem(self.x + dx + NX, NX) * 2 + c


class Wires:
    def __init__(self, send_sem, recv_sem):
        self.send_sem, self.recv_sem = send_sem, recv_sem
        self.count = 0
        self.sent = []

    def send(self, src, dst, device):
        k = self.count
        self.count += 1
        assert k < NSEM
        copy = pltpu.make_async_remote_copy(
            src_ref=src,
            dst_ref=dst,
            send_sem=self.send_sem.at[k],
            recv_sem=self.recv_sem.at[k],
            device_id=device,
            device_id_type=pl.DeviceIdType.MESH,
        )
        copy.start()
        self.sent.append(copy)
        return copy

    def drain(self):
        for copy in self.sent:
            copy.wait_send()


TOP, BOTTOM = pl.ds(0, H), pl.ds(H, H)
WAYS = ((1, TOP), (-1, BOTTOM))


def gather_dp(w, p, own, buf, t):
    got = {}

    def start():
        for way, _ in WAYS:
            got["A", 1, way] = w.send(own, buf.at[p.j], p.device(dz=way))
        got["B", 0] = w.send(own, buf.at[p.j], p.device(dy=1))

    def pass_a(s):
        def run():
            for way, half in WAYS:
                got["A", s, way].wait_recv()
                block = buf.at[p.dp(-s * way)]
                if s < 3:
                    got["A", s + 1, way] = w.send(block, block, p.device(dz=way))
                else:
                    part = block.at[half]
                    got["A", 4, way] = w.send(part, part, p.device(dz=way))
                    got["F", 3, way] = w.send(block, block, p.device(dy=1))

        return run

    def pass_b(s):
        def run():
            if s == 0:
                got["B", 0].wait_recv()
            for way, _ in WAYS:
                if s > 0:
                    got["B", s, way].wait_recv()
                block = buf.at[p.dp(-s * way, 1)]
                if s < 2:
                    got["B", s + 1, way] = w.send(block, block, p.device(dz=way))

        return run

    def pass_far():
        for way, half in WAYS:
            got["A", 4, way].wait_recv()
            part = buf.at[p.dp(4)].at[half]
            got["F", 4, way] = w.send(part, part, p.device(dy=1))

    def last(s):
        def run():
            for way, _ in WAYS:
                got["F", s, way].wait_recv()

        return run

    steps = (start, pass_a(1), pass_b(0), pass_a(2), pass_b(1), pass_a(3), pass_b(2), pass_far, last(3), last(4))
    return list(zip(t, steps))


def gather_mp(w, p, own, buf, t):
    got = {}

    def over(key, ref):
        got["C", key] = w.send(ref, ref, p.device(dc=1))

    def start():
        got["C", "own"] = w.send(own, buf.at[p.i], p.device(dc=1))
        got["B", 0] = w.send(own, buf.at[p.i], p.device(dh=1))
        for way, _ in WAYS:
            got["A", 1, way] = w.send(own, buf.at[p.i], p.device(dx=way))

    def near(name, h):
        def run():
            for way, half in WAYS:
                got[name, 1, way].wait_recv()
                block = buf.at[p.mp(h, -way)]
                part = block.at[half]
                got[name, 2, way] = w.send(part, part, p.device(dx=way))
                over((name, 1, way), block)

        return run

    def partner():
        got["B", 0].wait_recv()
        block = buf.at[p.mp(1)]
        for way, _ in WAYS:
            got["B", 1, way] = w.send(block, block, p.device(dx=way))
        over(("B", 0), block)

    def far(name, h):
        def run():
            for way, half in WAYS:
                got[name, 2, way].wait_recv()
                over((name, 2, way), buf.at[p.mp(h, 2)].at[half])

        return run

    def siblings():
        for key in list(got):
            if key[0] == "C":
                got[key].wait_recv()

    steps = (start, near("A", 0), partner, far("A", 0), near("B", 1), far("B", 1), siblings)
    return list(zip(t, steps))


def scatter_mp(w, p, term, done, bufs, t):
    send_c, got_c, send_x, got_x = bufs
    got = {}
    sides = ((1, 1), (0, 0))

    def start():
        for k in range(8):
            yh, x = k // 4, k % 4
            send_c[k] = term(p.mp(yh, x, 1)).astype(BF)
            got["C", k] = w.send(send_c.at[k], got_c.at[k], p.device(dc=1))

    def chip(h, dx):
        k = h * 4 + dx % 4
        return term(p.mp(h, dx)) + got_c[k].astype(F32)

    def far():
        for k in range(8):
            got["C", k].wait_recv()
        for h, s in sides:
            send_x[3 * s] = chip(h, 2).astype(BF)
            for way, half in WAYS:
                part = send_x.at[3 * s].at[half]
                got["far", h, way] = w.send(part, got_x.at[3 * s].at[half], p.device(dx=way))

    def near():
        for h, s in sides:
            for n, (way, half) in enumerate(WAYS):
                slot = 3 * s + 1 + n
                total = chip(h, way)
                got["far", h, way].wait_recv()
                low = got_x[3 * s, half].astype(F32)
                send_x[slot] = total.astype(BF)
                send_x[slot, half] = (total[half.start : half.start + H] + low).astype(BF)
                got["near", h, way] = w.send(send_x.at[slot], got_x.at[slot], p.device(dx=way))

    def arrived(h):
        total = chip(h, 0)
        for n, (way, _) in enumerate(WAYS):
            got["near", h, way].wait_recv()
            total = total + got_x[3 * h + 1 + n].astype(F32)
        return total

    def partner():
        send_x[6] = arrived(1).astype(BF)
        got["y"] = w.send(send_x.at[6], got_x.at[6], p.device(dh=1))

    def finish():
        total = arrived(0)
        got["y"].wait_recv()
        done(total + got_x[6].astype(F32))

    return list(zip(t, (start, far, near, partner, finish)))


def scatter_dp(w, p, term, done, bufs, t):
    send, got_ref = bufs
    got = {}

    def put(slot, value, device):
        send[slot] = value.astype(BF)
        got[slot] = w.send(send.at[slot], got_ref.at[slot], device)

    def take(slot):
        got[slot].wait_recv()
        return got_ref[slot].astype(F32)

    def start():
        put(12, term(p.dp(4, 1)), p.device(dy=1))
        for n, (way, _) in enumerate(WAYS):
            put(7 + n, term(p.dp(2 * way, 1)), p.device(dz=way))
        for n, (way, _) in enumerate(WAYS):
            put(13 + n, term(p.dp(3 * way, 1)), p.device(dy=1))

    def a4():
        send[0] = (term(p.dp(4)) + take(12)).astype(BF)
        for way, half in WAYS:
            got["half", way] = w.send(send.at[0].at[half], got_ref.at[0].at[half], p.device(dz=way))

    def b1():
        for n, (way, _) in enumerate(WAYS):
            put(9 + n, term(p.dp(way, 1)) + take(7 + n), p.device(dz=way))

    def a3():
        for n, (way, half) in enumerate(WAYS):
            total = term(p.dp(3 * way)) + take(13 + n)
            got["half", way].wait_recv()
            low = got_ref[0, half].astype(F32)
            send[1 + n] = total.astype(BF)
            send[1 + n, half] = (total[half.start : half.start + H] + low).astype(BF)
            got[1 + n] = w.send(send.at[1 + n], got_ref.at[1 + n], p.device(dz=way))

    def a2():
        for n, (way, _) in enumerate(WAYS):
            put(3 + n, term(p.dp(2 * way)) + take(1 + n), p.device(dz=way))

    def b0():
        put(11, term(p.dp(0, 1)) + take(9) + take(10), p.device(dy=1))

    def a1():
        for n, (way, _) in enumerate(WAYS):
            put(5 + n, term(p.dp(way)) + take(3 + n), p.device(dz=way))

    def finish():
        done(term(p.dp(0)) + take(11) + take(5) + take(6))

    return list(zip(t, (start, a4, b1, a3, a2, b0, a1, finish)))


def kernel(
    g, m1, m2, lf, rf, ql, qr,
    o_m1, o_m2, o_l, o_r, o_u,
    gb, qlb, qrb, tb, gtb,
    g_turned, ql_turned, t_own, d_turned, back,
    acc_t, acc_rot, acc_l,
    cs_b, cg_b, xs_b, xg_b, cs_r, cg_r, xs_r, xg_r, zs, zg,
    send_sem, recv_sem,
):
    p = Place()
    w = Wires(send_sem, recv_sem)
    across = {"dp": p.i, "mp": p.j}
    apart = p.i != p.j
    peers = [p.device(dz=1), p.device(dz=-1), p.device(dy=1), p.device(dh=1), p.device(dx=1), p.device(dx=-1), p.device(dc=1)]

    barrier = pltpu.get_barrier_semaphore()
    for peer in peers:
        pl.semaphore_signal(barrier, inc=1, device_id=peer, device_id_type=pl.DeviceIdType.MESH)

    @pl.when(apart)
    def _():
        pl.semaphore_signal(barrier, inc=1, device_id=across, device_id_type=pl.DeviceIdType.MESH)

    pl.semaphore_wait(barrier, jnp.where(apart, 8, 7))

    turn = pltpu.make_async_remote_copy(
        src_ref=g_turned,
        dst_ref=gtb.at[p.j],
        send_sem=send_sem.at[NSEM],
        recv_sem=recv_sem.at[NSEM],
        device_id=across,
        device_id_type=pl.DeviceIdType.MESH,
    )

    def prepare():
        g_turned[...] = turned(g[...]).astype(BF)

        @pl.when(apart)
        def _():
            turn.start()

        @pl.when(jnp.logical_not(apart))
        def _():
            gtb[p.i] = g_turned[...]

        gb[p.j] = g[...]
        qrb[p.i] = qr[...]
        ql_turned[...] = turned(ql[...]).astype(BF)
        qlb[p.j] = ql_turned[...]

    def turn_arrived():
        @pl.when(apart)
        def _():
            turn.wait()

    def product_t(first, count, fresh):
        def run():
            if fresh:
                acc_t[...] = jnp.zeros_like(acc_t)

            def body(n, _):
                k = lax.rem(p.z + first + n // 2, NZ) * 2 + n % 2
                acc_t[...] += dot(gb[k], qrb[k])
                return 0

            lax.fori_loop(0, count, body, 0)
            if not fresh:
                t_own[...] = acc_t[...].astype(BF)
                tb[p.i] = t_own[...]

        return run

    def product_l():
        acc_l[...] = jnp.zeros_like(acc_l)

        def body(k, _):
            acc_l[...] += dot(gb[k], gtb[k])
            return 0

        lax.fori_loop(0, 16, body, 0)
        o_l[...] = decay_factor * lf[...] + (1.0 - decay_factor) * acc_l[...]

    def moments():
        acc_rot[...] = jnp.zeros_like(acc_rot)

        def body(k, _):
            acc_rot[...] += dot(qlb[k], tb[k])
            return 0

        lax.fori_loop(0, 16, body, 0)
        rotated = acc_rot[...]
        first = decay_moment * m1[...] + (1.0 - decay_moment) * rotated
        second = decay_moment * m2[...] + (1.0 - decay_moment) * rotated * rotated
        o_m1[...] = first
        o_m2[...] = second
        direction = (first / (jnp.sqrt(second) + epsilon)).astype(BF)
        d_turned[...] = turned(direction).astype(BF)

    def back_done(total):
        back[...] = total.astype(BF)

    def right_done(total):
        o_r[...] = decay_factor * rf[...] + (1.0 - decay_factor) * total.T

    def update_done(total):
        o_u[...] = total.T.astype(BF)

    def back_term(k):
        return dot(d_turned[...], qlb[k])

    def right_term(k):
        return dot(g_turned[...], gb[k])

    def update_term(k):
        return dot(qrb[k], back[...])

    plan = []
    plan += gather_dp(w, p, g, gb, (0, 4.8, 4.9, 10, 12, 15, 18, 19, 20, 23))
    plan += gather_mp(w, p, qr, qrb, (0.1, 4.95, 6, 9, 10.5, 13.5, 14.5))
    plan += [(0.2, prepare), (7.9, turn_arrived)]
    plan += gather_dp(w, p, ql_turned, qlb, (0.3, 15.2, 15.3, 22, 23.8, 28, 29, 31, 32, 34))
    plan += gather_mp(w, p, gtb.at[p.i], gtb, (8, 14, 15.1, 19.1, 19.5, 22.5, 23.5))
    plan += [(18.5, product_t(6, 10, True)), (23.6, product_t(3, 6, False))]
    plan += gather_mp(w, p, t_own, tb, (23.7, 28.5, 29.5, 32.5, 33, 36.5, 37.5))
    plan += [(25, product_l), (38, moments)]
    plan += scatter_mp(w, p, back_term, back_done, (cs_b, cg_b, xs_b, xg_b), (39, 42, 45.5, 51, 55))
    plan += scatter_dp(w, p, update_term, update_done, (zs, zg), (56, 61, 61.5, 64.5, 69, 70, 74, 79))
    plan += scatter_mp(w, p, right_term, right_done, (cs_r, cg_r, xs_r, xg_r), (26, 57, 62, 67, 71))
    for _, step in sorted(plan, key=lambda item: item[0]):
        step()
    w.drain()


def per_device(gradient, first_moment, second_moment, left_factor, right_factor, left_basis, right_basis):
    ins = [a.reshape(N, N) for a in (gradient, first_moment, second_moment, left_factor, right_factor, left_basis, right_basis)]
    vmem = pl.BlockSpec(memory_space=pltpu.VMEM)
    block = pltpu.VMEM((N, N), BF)
    wide = pltpu.VMEM((N, N), F32)
    whole = pltpu.VMEM((16, N, N), BF)
    scatter = [pltpu.VMEM((8, N, N), BF)] * 2 + [pltpu.VMEM((7, N, N), BF)] * 2
    outs = pl.pallas_call(
        kernel,
        name="soap",
        out_shape=[jax.ShapeDtypeStruct((N, N), F32)] * 4 + [jax.ShapeDtypeStruct((N, N), BF)],
        in_specs=[vmem] * 7,
        out_specs=[vmem] * 5,
        scratch_shapes=[whole] * 5
        + [block] * 5
        + [wide] * 3
        + scatter * 2
        + [pltpu.VMEM((15, N, N), BF)] * 2
        + [pltpu.SemaphoreType.DMA((NSEM + 1,))] * 2,
        compiler_params=pltpu.CompilerParams(collective_id=0, has_side_effects=True, vmem_limit_bytes=60 * 1024 * 1024),
    )(*ins)
    return tuple(o.reshape(1, N, N) for o in outs)


def solution(mesh):
    spec = P(None, "mp", "dp")
    return jax.shard_map(
        per_device,
        mesh=mesh,
        in_specs=(spec,) * 5 + (P(None, "dp", "mp"), spec),
        out_specs=(spec,) * 5,
        check_vma=False,
    )
```

```python
import jax
import jax.numpy as jnp
from jax import lax
from jax.experimental import pallas as pl
from jax.experimental.pallas import tpu as pltpu
from jax.sharding import PartitionSpec as P

decay_moment = 0.95
decay_factor = 0.95
epsilon = 1e-08
N = 256
NZ = 8
NX = 4
NY = 4
NSEND = 19
NRECV = 133

BF = jnp.bfloat16
F32 = jnp.float32
MESH = pl.DeviceIdType.MESH
TIMES = {
    "mi": (0.00,),
    "hg": (0.02,),
    "hq": (1.54,),
    "hl": (2.18,),
    "mm": (34.45,),
    "hm": (34.67,),
    "gz": (2.12, 5.13, 5.87, 6.54, 7.24, 8.15, 8.88, 9.58, 10.29, 11.16, 11.89, 12.60, 13.30, 14.17, 14.90, 15.60, 16.31, 11.46, 17.45,),
    "qp": (2.06, 5.79, 7.19, 8.81, 11.62, 13.73, 12.33, 17.95, 18.65,),
    "lz": (16.00, 20.04, 20.08, 20.42, 21.12, 23.06, 23.79, 24.46, 25.17, 26.07, 26.80, 27.51, 28.21, 29.08, 29.81, 30.51, 31.22, 26.35, 32.30,),
    "t": (18.67, 19.39,),
    "tp": (19.98, 23.71, 25.12, 27.23, 30.04, 32.15, 30.74, 34.96, 35.66,),
    "r": (32.32, 35.68, 36.32,),
    "b0": (36.57, 37.12, 40.22, 40.92, 43.38, 41.33, 48.66, 51.74,),
    "b1": (37.59, 38.14, 41.65, 42.33, 46.20, 42.68, 49.01, 52.72,),
    "u0": (51.82, 52.16, 52.39, 53.70, 53.98, 54.44, 53.77, 53.82, 56.80, 56.86, 59.85, 60.55, 62.89, 63.59, 65.93, 66.64,),
    "u1": (52.80, 53.14, 53.37, 54.94, 55.26, 55.75, 55.06, 55.00, 58.21, 58.27, 61.25, 61.96, 64.30, 65.00, 67.34, 68.04,),
    "gp": (10.99, 15.92, 32.96, 22.38, 29.41, 33.63, 38.61, 33.55, 38.63,),
    "ls": (38.65, 38.99, 39.22, 41.04, 41.60, 42.58, 41.11, 41.22, 41.16, 41.27, 44.15, 44.85, 44.21, 44.91, 47.19, 48.60, 47.89, 50.44, 50.50, 51.64, 50.94, 54.03, 54.19, 55.59, 54.89, 57.56,),
    "rp": (49.27, 49.92, 53.88, 54.55, 57.66, 55.31, 63.99, 67.77,),
    "rr": (46.61,),
    "rl": (57.61,),
    "rt": (67.85,),
    "ru": (68.09,),
}


def dot(a, b):
    return jnp.dot(a, b, preferred_element_type=F32)


def turned(a):
    return a.astype(F32).T


class Place:
    def __init__(self):
        j, i = lax.axis_index("dp"), lax.axis_index("mp")
        self.z, self.y = j // 2, (i // 8) * 2 + j % 2
        self.x, self.c = (i // 2) % NX, i % 2
        self.away = j % 2 != self.c

    def row(self, dy=0, dx=0):
        y = lax.rem(self.y + dy + NY, NY)
        return (y // 2) * 8 + lax.rem(self.x + dx + NX, NX) * 2 + y % 2

    def column(self, dz=0, dc=0):
        return lax.rem(self.z + dz + NZ, NZ) * 2 + (1 - self.c if dc else self.c)

    def device(self, dz=0, dy=0, dx=0, dc=0):
        y = lax.rem(self.y + dy + NY, NY)
        c = 1 - self.c if dc else self.c
        z, x = lax.rem(self.z + dz + NZ, NZ), lax.rem(self.x + dx + NX, NX)
        return {"dp": z * 2 + y % 2, "mp": (y // 2) * 8 + x * 2 + c}

    def twin(self):
        y = self.y + 1 - 2 * (self.y % 2)
        return {"dp": self.z * 2 + y % 2, "mp": (y // 2) * 8 + self.x * 2 + 1 - self.c}


class Wires:
    def __init__(self, send_sem, recv_sem):
        self.send_sem, self.recv_sem = send_sem, recv_sem
        self.sends = self.recvs = 0

    def flow(self, gauge):
        self.sends += 1
        assert self.sends <= NSEND
        return Flow(self, self.send_sem.at[self.sends - 1], gauge)

    def receiver(self):
        self.recvs += 1
        assert self.recvs <= NRECV
        return self.recv_sem.at[self.recvs - 1]


class Flow:
    def __init__(self, wires, send_sem, gauge):
        self.wires, self.send_sem, self.gauge = wires, send_sem, gauge
        self.groups = {}

    def send(self, group, src, dst, device):
        if group not in self.groups:
            self.groups[group] = self.wires.receiver()
        pltpu.make_async_remote_copy(
            src_ref=src,
            dst_ref=dst,
            send_sem=self.send_sem,
            recv_sem=self.groups[group],
            device_id=device,
            device_id_type=MESH,
        ).start()

    def pause(self, sem, quarters):
        if quarters >= 4:
            assert quarters % 4 == 0
            size = self.gauge.at[pl.ds(0, quarters // 4)]
        else:
            size = self.gauge.at[0, pl.ds(0, quarters * 64)]
        pltpu.make_async_copy(size, size, sem).wait()

    def wait(self, group, quarters):
        self.pause(self.groups[group], quarters)

    def drain(self):
        self.pause(self.send_sem, 60)


WAYS = (1, -1)


def half(f):
    return pl.ds(f * 128, 128)


def quarter(f, way):
    return pl.ds(f * 128 + (0 if way == 1 else 64), 64)


def part(h):
    return pl.ds(h * 64, 64)


def along(f, a=0, b=0):
    return {"dy": a, "dx": b} if f == 0 else {"dy": b, "dx": a}


def gather_z(w, p, own, buf):
    def start():
        for h in range(4):
            for way in WAYS:
                w.send((1, h), own.at[part(h)], buf.at[p.column(), part(h)], p.device(dz=way))
        w.send("C near", own, buf.at[p.column()], p.device(dc=1))

    def arrive(n, h):
        last = WAYS[h // 2]

        def step():
            w.wait((n, h), 2 if n < 4 else 1)
            for way in WAYS if n < 4 else (last,):
                ref = buf.at[p.column(-n * way), part(h)]
                if n < 3 or (n == 3 and way == last):
                    w.send((n + 1, h), ref, ref, p.device(dz=way))
            for way in WAYS if n < 4 else (last,):
                ref = buf.at[p.column(-n * way), part(h)]
                w.send("C near" if n < 3 else "C far", ref, ref, p.device(dc=1))

        return step

    def near_siblings():
        w.wait("C near", 4 * 5)

    def far_siblings():
        w.wait("C far", 4 * 3)

    return [start] + [arrive(n, h) for n in (1, 2, 3, 4) for h in range(4)] + [near_siblings, far_siblings]


def gather_plane(w, p, own, buf):
    def send(group, f, ref, dst=None, **to):
        w.send(group, ref, ref if dst is None else dst, p.device(**along(f, **to)))

    def block(f, a, b, rows):
        return buf.at[p.row(**along(f, a, b)), rows]

    def start():
        for stage in ("a", "b"):
            for f in (0, 1):
                for way in WAYS:
                    dst = buf.at[p.row(), half(f)]
                    if stage == "a":
                        send("a1", f, own.at[half(f)], dst, a=way)
                    else:
                        send(("b", 0), f, own.at[half(f)], dst, b=way)

    def first():
        w.wait("a1", 8)
        for f in (0, 1):
            for way in WAYS:
                send("a2", f, block(f, -way, 0, quarter(f, way)), a=way)
        for f in (0, 1):
            for way in WAYS:
                for v in WAYS:
                    send(("b", 1), f, block(f, -way, 0, half(f)), b=v)

    def second(q):
        def step():
            w.wait(("b", q), 8 if q != 1 else 16)
            for r in (1, -1) if q == 1 else (q,):
                for f in (0, 1):
                    for v in WAYS:
                        send(("bb", q), f, block(f, r, -v, quarter(f, v)), b=v)

        return step

    def opposite():
        w.wait("a2", 4)
        for f in (0, 1):
            for v in WAYS:
                send(("b", 2), f, block(f, 2, 0, half(f)), b=v)

    def last(q):
        def step():
            w.wait(("bb", q), 4 if q != 1 else 8)

        return step

    return [start, first, second(0), opposite, second(1), second(2), last(0), last(1), last(2)]


def scatter_plane(w, p, term, done, bufs):
    base, out, into = bufs
    early = [(dy, dx) for dy in range(4) for dx in range(4) if dy == 2 or dx == 2]
    late = [(dy, dx) for dy in range(4) for dx in range(4) if dy != 2 and dx != 2]

    def terms(places):
        for dy, dx in places:
            base[dy * 4 + dx] = term(p.row(dy, dx))

    def held(f, a, b, rows):
        d = along(f, a, b)
        return base[(d["dy"] % 4) * 4 + d["dx"] % 4, rows]

    def send(group, f, slot, rows, **to):
        w.send(group, out.at[slot, rows], into.at[slot, rows], p.device(**along(f, **to)))

    def far():
        terms(early)
        for q in (2, 1, -1, 0):
            for f in (0, 1):
                out[q % 4, half(f)] = held(f, q, 2, half(f)).astype(BF)
        for q in (2, 1, -1, 0):
            for f in (0, 1):
                for v in WAYS:
                    send((2, abs(q)), f, q % 4, quarter(f, v), b=v)

    def rest():
        terms(late)

    def near(q):
        def step():
            w.wait((2, q), 4 if q != 1 else 8)
            for r in (1, -1) if q == 1 else (q,):
                for f in (0, 1):
                    for n, v in enumerate(WAYS):
                        slot, rows = 4 + (r % 4) * 2 + n, quarter(f, v)
                        out[slot, half(f)] = held(f, r, v, half(f)).astype(BF)
                        out[slot, rows] = (held(f, r, v, rows) + into[r % 4, rows].astype(F32)).astype(BF)
                        send((1, q), f, slot, half(f), b=v)

        return step

    def line(f, q, rows):
        total = held(f, q, 0, rows)
        for n, v in enumerate(WAYS):
            total = total + into[4 + (q % 4) * 2 + n, rows].astype(F32)
        return total

    def opposite():
        w.wait((1, 2), 8)
        for f in (0, 1):
            out[12, half(f)] = line(f, 2, half(f)).astype(BF)
            for way in WAYS:
                send("a2", f, 12, quarter(f, way), a=way)

    def beside():
        w.wait((1, 1), 16)
        w.wait("a2", 4)
        for f in (0, 1):
            for n, way in enumerate(WAYS):
                rows = quarter(f, way)
                out[13 + n, half(f)] = line(f, way, half(f)).astype(BF)
                out[13 + n, rows] = (line(f, way, rows) + into[12, rows].astype(F32)).astype(BF)
                send("a1", f, 13 + n, half(f), a=way)

    def finish():
        w.wait((1, 0), 8)
        w.wait("a1", 8)
        for f in (0, 1):
            total = line(f, 0, half(f))
            for n in (0, 1):
                total = total + into[13 + n, half(f)].astype(F32)
            done(f, total)

    return [far, rest, near(2), near(1), opposite, near(0), beside, finish]


def scatter_z(w, p, term, done, bufs, parts=2):
    base, mate_out, mate_in, out, into = bufs
    stages = ((4, 3, 5), (2, 6), (1, 7, 0))
    size = N // parts

    def rows(h):
        return pl.ds(h * size, size)

    def slot(n, way):
        return 0 if n == 4 else 1 + (n - 1) * 2 + (0 if way == 1 else 1)

    def start(k):
        def step():
            for dz in stages[k]:
                mate_out[dz] = term(p.column(dz, 1)).astype(BF)
            for dz in stages[k]:
                w.send(("C", k), mate_out.at[dz], mate_in.at[dz], p.device(dc=1))
            for dz in stages[k]:
                base[dz] = term(p.column(dz))

        return step

    def chip(k):
        def step():
            w.wait(("C", k), 4 * len(stages[k]))
            for dz in stages[k]:
                base[dz] = base[dz] + mate_in[dz].astype(F32)

        return step

    def push(n, h):
        last = WAYS[h // (parts // 2)]

        def step():
            if n < 3:
                w.wait((n + 1, h), 8 // parts)
            if n == 3:
                w.wait((4, h), 4 // parts)
            for way in WAYS if n < 4 else (last,):
                total = base[(n * way) % 8, rows(h)]
                if n < 3 or (n == 3 and way == last):
                    total = total + into[slot(n + 1, way), rows(h)].astype(F32)
                out[slot(n, way), rows(h)] = total.astype(BF)
                w.send((n, h), out.at[slot(n, way), rows(h)], into.at[slot(n, way), rows(h)], p.device(dz=way))

        return step

    def finish(h):
        def step():
            w.wait((1, h), 8 // parts)
            total = base[0, rows(h)]
            for way in WAYS:
                total = total + into[slot(1, way), rows(h)].astype(F32)
            done(rows(h), total)

        return step

    steps = [start(0), start(1), start(2), chip(0), chip(1), chip(2)]
    return steps + [push(n, h) for n in (4, 3, 2, 1) for h in range(parts)] + [finish(h) for h in range(parts)]


def kernel(
    g_in, m1_in, m2_in, ql_in, qr_in,
    o_rot, o_l, o_r, o_u,
    g_0, ql_0, qr_0, m1_0, m2_0, mm_0, mm,
    g, ql, qr,
    gb, qlb, qrb, tb, gcb,
    g_turned, ql_turned, t_own, d_turned, u_0, u_1,
    left, left_1, right, right_1, rot_0, rot_1,
    acc_t, rot, right_sum,
    back_0, back_1,
    pb_0, po_0, pi_0, pb_1, po_1, pi_1, pb_r, po_r, pi_r,
    zb_0, zmo_0, zmi_0, zo_0, zi_0, zb_1, zmo_1, zmi_1, zo_1, zi_1, zb_l, zmo_l, zmi_l, zo_l, zi_l,
    send_sem, recv_sem, load_sem,
):
    p = Place()
    w = Wires(send_sem, recv_sem)
    home = jnp.logical_not(p.away)
    peers = [p.device(dz=1), p.device(dz=-1), p.device(dy=1), p.device(dy=-1), p.device(dx=1), p.device(dx=-1), p.device(dc=1), p.twin()]

    barrier = pltpu.get_barrier_semaphore()
    for peer in peers:
        pl.semaphore_signal(barrier, inc=1, device_id=peer, device_id_type=MESH)

    loads = {}
    for n, (name, src, dst) in enumerate((("g", g_in, g_0), ("qr", qr_in, qr_0), ("ql", ql_in, ql_0), ("m1", m1_in, m1_0), ("m2", m2_in, m2_0))):
        loads[name] = pltpu.make_async_copy(src, dst, load_sem.at[n])
        loads[name].start()
    loads["g"].wait()
    loads["qr"].wait()
    pl.semaphore_wait(barrier, 8)

    moves = {}

    def move(name, src, dst):
        copy = pltpu.make_async_remote_copy(
            src_ref=src,
            dst_ref=dst,
            send_sem=w.flow(None).send_sem,
            recv_sem=w.receiver(),
            device_id=p.twin(),
            device_id_type=MESH,
        )
        moves[name] = copy

        @pl.when(p.away)
        def _():
            copy.start()

        @pl.when(home)
        def _():
            dst[...] = src[...]

    def moved(name):
        @pl.when(p.away)
        def _():
            moves[name].wait_recv()

    def move_in():
        move("g", g_0, g)
        move("qr", qr_0, qr)
        loads["ql"].wait()
        move("ql", ql_0, ql)

    def have_g():
        moved("g")

    def have_qr():
        moved("qr")

    def have_ql():
        gb[p.column()] = g[...]
        gcb[p.row()] = g[...]
        qrb[p.row()] = qr[...]
        moved("ql")
        ql_turned[...] = turned(ql[...]).astype(BF)
        qlb[p.column()] = ql_turned[...]

    def move_moments():
        loads["m1"].wait()
        loads["m2"].wait()
        mm_0[0] = m1_0[...].astype(BF)
        mm_0[1] = m2_0[...].astype(BF)
        move("m", mm_0, mm)
        g_turned[...] = turned(g[...]).astype(BF)

    def have_moments():
        moved("m")

    def gathered(acc, lefts, rights, keys, fresh):
        total = None if fresh else acc[...]
        for k in keys:
            term = dot(lefts[k], rights[k])
            total = term if total is None else total + term
        acc[...] = total

    def product_t(dzs, fresh=False, last=False):
        def product():
            gathered(acc_t, gb, qrb, [p.column(dz, dc) for dz in dzs for dc in (0, 1)], fresh)
            if last:
                t_own[...] = acc_t[...].astype(BF)
                tb[p.row()] = t_own[...]

        return product

    def rotate(keys, fresh=False):
        def rotated():
            gathered(rot, qlb, tb, [p.row(dy, dx) for dy, dx in keys], fresh)

        return rotated

    def moments():
        rotated = rot[...]
        first = decay_moment * mm[0].astype(F32) + (1.0 - decay_moment) * rotated
        second = decay_moment * mm[1].astype(F32) + (1.0 - decay_moment) * rotated * rotated
        direction = (first / (jnp.sqrt(second) + epsilon)).astype(BF)
        d_turned[...] = turned(direction).astype(BF)

    def left_term(k):
        return lax.dot_general(g[...], gcb[k], (((1,), (1,)), ((), ())), preferred_element_type=F32)

    def left_done(h, total):
        left[h] = total.astype(BF)

    def right_done(f, total):
        right_sum[half(f)] = total

    def right_term(k):
        return dot(g_turned[...], gb[k])

    backs = (back_0, back_1)

    def back_term(n):
        return lambda k: dot(d_turned[...], qlb[k, :, half(n)])

    def back_done(n):
        def store(f, total):
            backs[n][half(f)] = total.astype(BF)

        return store

    def update_term(n):
        return lambda k: dot(qrb[k], backs[n][...])

    def update_done(n):
        def store(rows, total):
            acc_t[rows, half(n)] = total

        return store

    def return_rotated():
        rot_0[...] = rot[...].astype(BF)
        move("rot", rot_0, rot_1)

    def return_right():
        right[...] = right_sum[...].T.astype(BF)
        move("right", right, right_1)

    def return_left():
        move("left", left, left_1)

    def return_update():
        u_0[...] = acc_t[...].T.astype(BF)
        move("u", u_0, u_1)

    def results():
        for name, src, dst in (("rot", rot_1, o_rot), ("right", right_1, o_r), ("left", left_1, o_l), ("u", u_1, o_u)):
            moved(name)
            dst[...] = src[...].astype(dst.dtype)

    near_rows = [(0, 0), (1, 0), (3, 0), (0, 1), (0, 3), (1, 1), (3, 1), (1, 3), (3, 3)]
    far_rows = [(2, 0), (0, 2), (2, 1), (2, 3), (1, 2), (3, 2), (2, 2)]
    gauge = {"gz": gb, "qp": qrb, "lz": qlb, "tp": tb, "b0": po_0, "b1": po_1, "u0": po_0, "u1": po_1, "gp": gcb, "ls": po_r, "rp": po_r}
    f = {name: w.flow(ref) for name, ref in gauge.items()}
    flows = {
        "mi": [move_in],
        "hg": [have_g],
        "hq": [have_qr],
        "hl": [have_ql],
        "mm": [move_moments],
        "hm": [have_moments],
        "gz": gather_z(f["gz"], p, g, gb),
        "qp": gather_plane(f["qp"], p, qr, qrb),
        "lz": gather_z(f["lz"], p, ql_turned, qlb),
        "t": [product_t([0, 1, 7, 2, 6], fresh=True), product_t([3, 5, 4], last=True)],
        "tp": gather_plane(f["tp"], p, t_own, tb),
        "r": [rotate(near_rows, fresh=True), rotate(far_rows), moments],
        "b0": scatter_plane(f["b0"], p, back_term(0), back_done(0), (pb_0, po_0, pi_0)),
        "b1": scatter_plane(f["b1"], p, back_term(1), back_done(1), (pb_1, po_1, pi_1)),
        "u0": scatter_z(f["u0"], p, update_term(0), update_done(0), (zb_0, zmo_0, zmi_0, zo_0, zi_0)),
        "u1": scatter_z(f["u1"], p, update_term(1), update_done(1), (zb_1, zmo_1, zmi_1, zo_1, zi_1)),
        "gp": gather_plane(f["gp"], p, g, gcb),
        "ls": scatter_z(f["ls"], p, left_term, left_done, (zb_l, zmo_l, zmi_l, zo_l, zi_l), parts=4),
        "rp": scatter_plane(f["rp"], p, right_term, right_done, (pb_r, po_r, pi_r)),
        "rr": [return_rotated],
        "rl": [return_left],
        "rt": [return_right],
        "ru": [return_update],
    }
    plan = [(t, step) for name, steps in flows.items() for t, step in zip(TIMES[name], steps, strict=True)]
    for _, step in sorted(plan, key=lambda item: item[0]):
        step()
    results()
    for flow in f.values():
        flow.drain()

    @pl.when(p.away)
    def _():
        for copy in moves.values():
            copy.wait_send()


def per_device(gradient, first_moment, second_moment, left_factor, right_factor, left_basis, right_basis):
    ins = [a.reshape(N, N) for a in (gradient, first_moment, second_moment, left_basis, right_basis)]
    block = pltpu.VMEM((N, N), BF)
    wide = pltpu.VMEM((N, N), F32)

    def many(n, dtype=BF, width=N):
        return pltpu.VMEM((n, N, width), dtype)

    rotated, left_sum, right_sum, update = pl.pallas_call(
        kernel,
        name="soap",
        out_shape=[jax.ShapeDtypeStruct((N, N), F32)] * 3 + [jax.ShapeDtypeStruct((N, N), BF)],
        in_specs=[pl.BlockSpec(memory_space=pl.ANY)] * 5,
        out_specs=[pl.BlockSpec(memory_space=pltpu.VMEM)] * 4,
        scratch_shapes=[block] * 3
        + [wide] * 2
        + [many(2)] * 2
        + [block] * 3
        + [many(16)] * 5
        + [block] * 12
        + [wide] * 3
        + [pltpu.VMEM((N, 128), BF)] * 2
        + ([many(16, F32, 128)] + [many(15, BF, 128)] * 2) * 2
        + [many(16, F32), many(15), many(15)]
        + ([many(8, F32, 128)] + [many(8, BF, 128)] * 2 + [many(7, BF, 128)] * 2) * 2
        + [many(8, F32), many(8), many(8), many(7), many(7)]
        + [pltpu.SemaphoreType.DMA((NSEND,)), pltpu.SemaphoreType.DMA((NRECV,))]
        + [pltpu.SemaphoreType.DMA((5,))],
        compiler_params=pltpu.CompilerParams(collective_id=0, has_side_effects=True, vmem_limit_bytes=60 * 1024 * 1024),
    )(*ins)
    rotated, left_sum, right_sum, update = (a.reshape(1, N, N) for a in (rotated, left_sum, right_sum, update))
    scale = 1.0 - decay_factor
    new_first = decay_moment * first_moment + (1.0 - decay_moment) * rotated
    new_second = decay_moment * second_moment + (1.0 - decay_moment) * rotated * rotated
    new_left = decay_factor * left_factor + scale * left_sum
    new_right = decay_factor * right_factor + scale * right_sum
    return (new_first, new_second, new_left, new_right, update)


def solution(mesh):
    spec = P(None, "mp", "dp")
    return jax.shard_map(
        per_device,
        mesh=mesh,
        in_specs=(spec,) * 5 + (P(None, "dp", "mp"), spec),
        out_specs=(spec,) * 5,
        check_vma=False,
    )
```

```python
import jax
import jax.numpy as jnp
from jax import lax
from jax.experimental import pallas as pl
from jax.experimental.pallas import tpu as pltpu
from jax.sharding import PartitionSpec as P

decay_moment = 0.95
decay_factor = 0.95
epsilon = 1e-08
N = 256
NZ = 8
NX = 4
NY = 4
NSEND = 22
NRECV = 136
LIMIT = 62

BF = jnp.bfloat16
F32 = jnp.float32
MESH = pl.DeviceIdType.MESH
TIMES = {
    "mi": (0.00,),
    "hg": (0.02,),
    "hq": (1.54,),
    "hl": (2.18,),
    "mm": (12.00,),
    "hm": (38.78,),
    "gz": (2.12, 5.13, 5.87, 6.54, 7.24, 8.15, 8.88, 9.58, 10.29, 11.16, 11.89, 12.60, 13.30, 16.81, 17.51, 16.83, 17.54, 11.46, 18.68,),
    "qp": (2.06, 5.79, 7.19, 10.73, 13.52, 15.63, 14.22, 19.83, 20.54,),
    "lz": (10.66, 15.50, 16.21, 16.91, 17.61, 20.02, 21.28, 21.91, 22.12, 24.53, 25.79, 26.49, 27.20, 29.04, 30.30, 31.00, 31.71, 23.30, 32.79,),
    "t": (20.56, 21.32,),
    "tp": (21.95, 26.16, 27.57, 29.68, 32.49, 34.60, 33.45, 37.50, 38.12,),
    "r": (32.81, 38.14, 38.80,),
    "b0": (39.05, 39.60, 42.37, 43.98, 45.90, 44.10, 49.76, 53.30,),
    "b1": (42.85, 43.40, 46.25, 46.95, 50.47, 47.30, 53.71, 56.79,),
    "u0": (53.38, 53.81, 54.04, 55.17, 55.50, 55.99, 55.35, 55.30, 55.24, 55.41, 60.38, 60.44, 65.31, 66.02, 68.83, 69.53,),
    "u1": (56.87, 57.21, 57.50, 58.67, 59.00, 59.49, 58.74, 58.85, 58.79, 58.91, 63.90, 64.61, 67.42, 68.13, 70.47, 71.17,),
    "gp": (4.65, 18.70, 18.00, 25.03, 32.06, 35.58, 22.74, 37.52, 40.32,),
    "ls": (40.34, 40.92, 41.58, 42.63, 43.87, 44.31, 42.75, 44.20, 44.26, 42.69, 43.92, 47.07, 46.35, 45.59, 48.69, 52.21, 51.51, 50.80, 53.24, 57.44, 58.09, 63.01, 57.91, 62.59, 63.30, 68.22,),
    "rp": (36.33, 36.98, 41.41, 54.38, 51.14, 51.85, 61.11, 66.39,),
    "rr": (57.83,),
    "rl": (68.27,),
    "rt": (66.47,),
    "ru": (71.22,),
}


def dot(a, b):
    return jnp.dot(a, b, preferred_element_type=F32)


def turned(a):
    return a.astype(F32).T


class Place:
    def __init__(self):
        j, i = lax.axis_index("dp"), lax.axis_index("mp")
        self.z, self.y = j // 2, (i // 8) * 2 + j % 2
        self.x, self.c = (i // 2) % NX, i % 2
        self.away = j % 2 != self.c

    def row(self, dy=0, dx=0):
        y = lax.rem(self.y + dy + NY, NY)
        return (y // 2) * 8 + lax.rem(self.x + dx + NX, NX) * 2 + y % 2

    def column(self, dz=0, dc=0):
        return lax.rem(self.z + dz + NZ, NZ) * 2 + (1 - self.c if dc else self.c)

    def device(self, dz=0, dy=0, dx=0, dc=0):
        y = lax.rem(self.y + dy + NY, NY)
        c = 1 - self.c if dc else self.c
        z, x = lax.rem(self.z + dz + NZ, NZ), lax.rem(self.x + dx + NX, NX)
        return {"dp": z * 2 + y % 2, "mp": (y // 2) * 8 + x * 2 + c}

    def twin(self):
        y = self.y + 1 - 2 * (self.y % 2)
        return {"dp": self.z * 2 + y % 2, "mp": (y // 2) * 8 + self.x * 2 + 1 - self.c}


class Wires:
    def __init__(self, send_sem, recv_sem):
        self.send_sem, self.recv_sem = send_sem, recv_sem
        self.sends = self.recvs = 0

    def flow(self, gauge):
        self.sends += 1
        assert self.sends <= NSEND
        return Flow(self, self.send_sem.at[self.sends - 1], gauge)

    def receiver(self):
        self.recvs += 1
        assert self.recvs <= NRECV
        return self.recv_sem.at[self.recvs - 1]


class Flow:
    def __init__(self, wires, send_sem, gauge):
        self.wires, self.send_sem, self.gauge = wires, send_sem, gauge
        self.groups = {}

    def send(self, group, src, dst, device):
        if group not in self.groups:
            self.groups[group] = self.wires.receiver()
        pltpu.make_async_remote_copy(
            src_ref=src,
            dst_ref=dst,
            send_sem=self.send_sem,
            recv_sem=self.groups[group],
            device_id=device,
            device_id_type=MESH,
        ).start()

    def pause(self, sem, quarters):
        if quarters >= 4:
            assert quarters % 4 == 0
            size = self.gauge.at[pl.ds(0, quarters // 4)]
        else:
            size = self.gauge.at[0, pl.ds(0, quarters * 64)]
        pltpu.make_async_copy(size, size, sem).wait()

    def wait(self, group, quarters):
        self.pause(self.groups[group], quarters)

    def drain(self):
        self.pause(self.send_sem, 60)


WAYS = (1, -1)


def half(f):
    return pl.ds(f * 128, 128)


def quarter(f, way):
    return pl.ds(f * 128 + (0 if way == 1 else 64), 64)


def part(h):
    return pl.ds(h * 64, 64)


def along(f, a=0, b=0):
    return {"dy": a, "dx": b} if f == 0 else {"dy": b, "dx": a}


def gather_z(w, p, own, buf):
    def start():
        for h in range(4):
            for way in WAYS:
                w.send((1, h), own.at[part(h)], buf.at[p.column(), part(h)], p.device(dz=way))
        w.send("C near", own, buf.at[p.column()], p.device(dc=1))

    def arrive(n, h):
        last = WAYS[h // 2]

        def step():
            w.wait((n, h), 2 if n < 4 else 1)
            for way in WAYS if n < 4 else (last,):
                ref = buf.at[p.column(-n * way), part(h)]
                if n < 3 or (n == 3 and way == last):
                    w.send((n + 1, h), ref, ref, p.device(dz=way))
            for way in WAYS if n < 4 else (last,):
                ref = buf.at[p.column(-n * way), part(h)]
                w.send("C near" if n < 3 else "C far", ref, ref, p.device(dc=1))

        return step

    def near_siblings():
        w.wait("C near", 4 * 5)

    def far_siblings():
        w.wait("C far", 4 * 3)

    return [start] + [arrive(n, h) for n in (1, 2, 3, 4) for h in range(4)] + [near_siblings, far_siblings]


def gather_plane(w, p, own, buf):
    def send(group, f, ref, dst=None, **to):
        w.send(group, ref, ref if dst is None else dst, p.device(**along(f, **to)))

    def block(f, a, b, rows):
        return buf.at[p.row(**along(f, a, b)), rows]

    def start():
        for stage in ("a", "b"):
            for f in (0, 1):
                for way in WAYS:
                    dst = buf.at[p.row(), half(f)]
                    if stage == "a":
                        send("a1", f, own.at[half(f)], dst, a=way)
                    else:
                        send(("b", 0), f, own.at[half(f)], dst, b=way)

    def first():
        w.wait("a1", 8)
        for f in (0, 1):
            for way in WAYS:
                send("a2", f, block(f, -way, 0, quarter(f, way)), a=way)
        for f in (0, 1):
            for way in WAYS:
                for v in WAYS:
                    send(("b", 1), f, block(f, -way, 0, half(f)), b=v)

    def second(q):
        def step():
            w.wait(("b", q), 8 if q != 1 else 16)
            for r in (1, -1) if q == 1 else (q,):
                for f in (0, 1):
                    for v in WAYS:
                        send(("bb", q), f, block(f, r, -v, quarter(f, v)), b=v)

        return step

    def opposite():
        w.wait("a2", 4)
        for f in (0, 1):
            for v in WAYS:
                send(("b", 2), f, block(f, 2, 0, half(f)), b=v)

    def last(q):
        def step():
            w.wait(("bb", q), 4 if q != 1 else 8)

        return step

    return [start, first, second(0), opposite, second(1), second(2), last(0), last(1), last(2)]


def scatter_plane(w, p, term, done, bufs):
    base, out, into = bufs
    early = [(dy, dx) for dy in range(4) for dx in range(4) if dy == 2 or dx == 2]
    late = [(dy, dx) for dy in range(4) for dx in range(4) if dy != 2 and dx != 2]

    def terms(places):
        for dy, dx in places:
            base[dy * 4 + dx] = term(p.row(dy, dx))

    def held(f, a, b, rows):
        d = along(f, a, b)
        return base[(d["dy"] % 4) * 4 + d["dx"] % 4, rows]

    def send(group, f, slot, rows, **to):
        w.send(group, out.at[slot, rows], into.at[slot, rows], p.device(**along(f, **to)))

    def far():
        terms(early)
        for q in (2, 1, -1, 0):
            for f in (0, 1):
                out[q % 4, half(f)] = held(f, q, 2, half(f)).astype(BF)
        for q in (2, 1, -1, 0):
            for f in (0, 1):
                for v in WAYS:
                    send((2, abs(q)), f, q % 4, quarter(f, v), b=v)

    def rest():
        terms(late)

    def near(q):
        def step():
            w.wait((2, q), 4 if q != 1 else 8)
            for r in (1, -1) if q == 1 else (q,):
                for f in (0, 1):
                    for n, v in enumerate(WAYS):
                        slot, rows = 4 + (r % 4) * 2 + n, quarter(f, v)
                        out[slot, half(f)] = held(f, r, v, half(f)).astype(BF)
                        out[slot, rows] = (held(f, r, v, rows) + into[r % 4, rows].astype(F32)).astype(BF)
                        send((1, q), f, slot, half(f), b=v)

        return step

    def line(f, q, rows):
        total = held(f, q, 0, rows)
        for n, v in enumerate(WAYS):
            total = total + into[4 + (q % 4) * 2 + n, rows].astype(F32)
        return total

    def opposite():
        w.wait((1, 2), 8)
        for f in (0, 1):
            out[12, half(f)] = line(f, 2, half(f)).astype(BF)
            for way in WAYS:
                send("a2", f, 12, quarter(f, way), a=way)

    def beside():
        w.wait((1, 1), 16)
        w.wait("a2", 4)
        for f in (0, 1):
            for n, way in enumerate(WAYS):
                rows = quarter(f, way)
                out[13 + n, half(f)] = line(f, way, half(f)).astype(BF)
                out[13 + n, rows] = (line(f, way, rows) + into[12, rows].astype(F32)).astype(BF)
                send("a1", f, 13 + n, half(f), a=way)

    def finish():
        w.wait((1, 0), 8)
        w.wait("a1", 8)
        for f in (0, 1):
            total = line(f, 0, half(f))
            for n in (0, 1):
                total = total + into[13 + n, half(f)].astype(F32)
            done(f, total)

    return [far, rest, near(2), near(1), opposite, near(0), beside, finish]


def scatter_z(w, p, term, done, bufs, parts=2):
    base, mate_out, mate_in, out, into = bufs
    stages = ((4, 3, 5), (2, 6), (1, 7, 0))
    size = N // parts

    def rows(h):
        return pl.ds(h * size, size)

    def slot(n, way):
        return 0 if n == 4 else 1 + (n - 1) * 2 + (0 if way == 1 else 1)

    def start(k):
        def step():
            for dz in stages[k]:
                mate_out[dz] = term(p.column(dz, 1)).astype(BF)
            for dz in stages[k]:
                w.send(("C", k), mate_out.at[dz], mate_in.at[dz], p.device(dc=1))
            for dz in stages[k]:
                base[dz] = term(p.column(dz))

        return step

    def chip(k):
        def step():
            w.wait(("C", k), 4 * len(stages[k]))
            for dz in stages[k]:
                base[dz] = base[dz] + mate_in[dz].astype(F32)

        return step

    def push(n, h):
        last = WAYS[h // (parts // 2)]

        def step():
            if n < 3:
                w.wait((n + 1, h), 8 // parts)
            if n == 2:
                w.wait((4, h), 4 // parts)
            for way in WAYS if n < 4 else (last,):
                total = base[(n * way) % 8, rows(h)]
                if n < 3:
                    total = total + into[slot(n + 1, way), rows(h)].astype(F32)
                if n == 2 and way == last:
                    total = total + into[0, rows(h)].astype(F32)
                out[slot(n, way), rows(h)] = total.astype(BF)
                to = p.device(dz=2 * way if n == 4 else way)
                w.send((n, h), out.at[slot(n, way), rows(h)], into.at[slot(n, way), rows(h)], to)

        return step

    def finish(h):
        def step():
            w.wait((1, h), 8 // parts)
            total = base[0, rows(h)]
            for way in WAYS:
                total = total + into[slot(1, way), rows(h)].astype(F32)
            done(rows(h), total)

        return step

    steps = [start(0), start(1), start(2), chip(0), chip(1), chip(2)]
    return steps + [push(n, h) for n in (4, 3, 2, 1) for h in range(parts)] + [finish(h) for h in range(parts)]


def kernel(
    g_in, m1_in, m2_in, ql_in, qr_in,
    o_rot, o_l, o_r, o_u,
    g_0, ql_0, qr_0, m1_0, m2_0, mm_0, mm,
    g, ql, qr,
    gb, qlb, qrb, tb, gcb,
    g_turned, ql_turned, t_own, d_turned, u_0, u_1,
    left, left_1, right, right_1, rot_0, rot_1,
    acc_t, rot, right_sum,
    back_0, back_1,
    pb_0, po_0, pi_0, pb_1, po_1, pi_1, pb_r, po_r, pi_r,
    zb_0, zmo_0, zmi_0, zo_0, zi_0, zb_1, zmo_1, zmi_1, zo_1, zi_1, zb_l, zmo_l, zmi_l, zo_l, zi_l,
    send_sem, recv_sem, load_sem,
):
    p = Place()
    w = Wires(send_sem, recv_sem)
    home = jnp.logical_not(p.away)
    peers = [p.device(dz=1), p.device(dz=-1), p.device(dy=1), p.device(dy=-1), p.device(dx=1), p.device(dx=-1), p.device(dc=1), p.twin()]
    peers += [p.device(dz=2), p.device(dz=-2), p.device(dx=2), p.device(dy=2)]

    barrier = pltpu.get_barrier_semaphore()
    for peer in peers:
        pl.semaphore_signal(barrier, inc=1, device_id=peer, device_id_type=MESH)

    loads = {}
    for n, (name, src, dst) in enumerate((("g", g_in, g_0), ("qr", qr_in, qr_0), ("ql", ql_in, ql_0), ("m1", m1_in, m1_0), ("m2", m2_in, m2_0))):
        loads[name] = pltpu.make_async_copy(src, dst, load_sem.at[n])
        loads[name].start()
    loads["g"].wait()
    loads["qr"].wait()
    pl.semaphore_wait(barrier, len(peers))

    moves = {}

    def move(name, src, dst):
        copy = pltpu.make_async_remote_copy(
            src_ref=src,
            dst_ref=dst,
            send_sem=w.flow(None).send_sem,
            recv_sem=w.receiver(),
            device_id=p.twin(),
            device_id_type=MESH,
        )
        moves[name] = copy

        @pl.when(p.away)
        def _():
            copy.start()

        @pl.when(home)
        def _():
            dst[...] = src[...]

    def moved(name):
        @pl.when(p.away)
        def _():
            moves[name].wait_recv()

    def move_in():
        move("g", g_0, g)
        move("qr", qr_0, qr)
        loads["ql"].wait()
        move("ql", ql_0, ql)

    def have_g():
        moved("g")

    def have_qr():
        moved("qr")

    def have_ql():
        gb[p.column()] = g[...]
        gcb[p.row()] = g[...]
        qrb[p.row()] = qr[...]
        moved("ql")
        ql_turned[...] = turned(ql[...]).astype(BF)
        qlb[p.column()] = ql_turned[...]

    def move_moments():
        loads["m1"].wait()
        loads["m2"].wait()
        mm_0[0] = m1_0[...].astype(BF)
        mm_0[1] = m2_0[...].astype(BF)
        move("m", mm_0, mm)
        g_turned[...] = turned(g[...]).astype(BF)

    def have_moments():
        moved("m")

    def gathered(acc, lefts, rights, keys, fresh):
        total = None if fresh else acc[...]
        for k in keys:
            term = dot(lefts[k], rights[k])
            total = term if total is None else total + term
        acc[...] = total

    def product_t(dzs, fresh=False, last=False):
        def product():
            gathered(acc_t, gb, qrb, [p.column(dz, dc) for dz in dzs for dc in (0, 1)], fresh)
            if last:
                t_own[...] = acc_t[...].astype(BF)
                tb[p.row()] = t_own[...]

        return product

    def rotate(keys, fresh=False):
        def rotated():
            gathered(rot, qlb, tb, [p.row(dy, dx) for dy, dx in keys], fresh)

        return rotated

    def moments():
        rotated = rot[...]
        first = decay_moment * mm[0].astype(F32) + (1.0 - decay_moment) * rotated
        second = decay_moment * mm[1].astype(F32) + (1.0 - decay_moment) * rotated * rotated
        direction = (first / (jnp.sqrt(second) + epsilon)).astype(BF)
        d_turned[...] = turned(direction).astype(BF)

    def left_term(k):
        return lax.dot_general(g[...], gcb[k], (((1,), (1,)), ((), ())), preferred_element_type=F32)

    def left_done(h, total):
        left[h] = total.astype(BF)

    def right_done(f, total):
        right_sum[half(f)] = total

    def right_term(k):
        return dot(g_turned[...], gb[k])

    backs = (back_0, back_1)

    def back_term(n):
        return lambda k: dot(d_turned[...], qlb[k, :, half(n)])

    def back_done(n):
        def store(f, total):
            backs[n][half(f)] = total.astype(BF)

        return store

    def update_term(n):
        return lambda k: dot(qrb[k], backs[n][...])

    def update_done(n):
        def store(rows, total):
            u_0[half(n), rows] = total.T.astype(BF)
            move(("u", n, rows.start), u_0.at[half(n), rows], u_1.at[half(n), rows])

        return store

    def return_rotated():
        rot_0[...] = rot[...].astype(BF)
        move("rot", rot_0, rot_1)

    def return_right():
        right[...] = right_sum[...].T.astype(BF)
        move("right", right, right_1)

    def return_left():
        move("left", left, left_1)

    def results():
        for name in moves:
            if name in ("rot", "right", "left") or name[0] == "u":
                moved(name)
        for src, dst in ((rot_1, o_rot), (right_1, o_r), (left_1, o_l), (u_1, o_u)):
            dst[...] = src[...]

    near_rows = [(0, 0), (1, 0), (3, 0), (0, 1), (0, 3), (1, 1), (3, 1), (1, 3), (3, 3)]
    far_rows = [(2, 0), (0, 2), (2, 1), (2, 3), (1, 2), (3, 2), (2, 2)]
    gauge = {"gz": gb, "qp": qrb, "lz": qlb, "tp": tb, "b0": po_0, "b1": po_1, "u0": po_0, "u1": po_1, "gp": gcb, "ls": po_r, "rp": po_r}
    f = {name: w.flow(ref) for name, ref in gauge.items()}
    flows = {
        "mi": [move_in],
        "hg": [have_g],
        "hq": [have_qr],
        "hl": [have_ql],
        "mm": [move_moments],
        "hm": [have_moments],
        "gz": gather_z(f["gz"], p, g, gb),
        "qp": gather_plane(f["qp"], p, qr, qrb),
        "lz": gather_z(f["lz"], p, ql_turned, qlb),
        "t": [product_t([0, 1, 7, 2, 6], fresh=True), product_t([3, 5, 4], last=True)],
        "tp": gather_plane(f["tp"], p, t_own, tb),
        "r": [rotate(near_rows, fresh=True), rotate(far_rows), moments],
        "b0": scatter_plane(f["b0"], p, back_term(0), back_done(0), (pb_0, po_0, pi_0)),
        "b1": scatter_plane(f["b1"], p, back_term(1), back_done(1), (pb_1, po_1, pi_1)),
        "u0": scatter_z(f["u0"], p, update_term(0), update_done(0), (zb_0, zmo_0, zmi_0, zo_0, zi_0)),
        "u1": scatter_z(f["u1"], p, update_term(1), update_done(1), (zb_1, zmo_1, zmi_1, zo_1, zi_1)),
        "gp": gather_plane(f["gp"], p, g, gcb),
        "ls": scatter_z(f["ls"], p, left_term, left_done, (zb_l, zmo_l, zmi_l, zo_l, zi_l), parts=4),
        "rp": scatter_plane(f["rp"], p, right_term, right_done, (pb_r, po_r, pi_r)),
        "rr": [return_rotated],
        "rl": [return_left],
        "rt": [return_right],
    }
    plan = [(t, step) for name, steps in flows.items() for t, step in zip(TIMES[name], steps, strict=True)]
    for _, step in sorted(plan, key=lambda item: item[0]):
        step()
    results()
    for flow in f.values():
        flow.drain()

    @pl.when(p.away)
    def _():
        for copy in moves.values():
            copy.wait_send()


def blend(rot, left, right, update, m1, m2, lf, rf, o_m1, o_m2, o_l, o_r, o_u):
    rotated = rot[...].astype(F32)
    scale = 1.0 - decay_factor
    o_m1[...] = decay_moment * m1[...] + (1.0 - decay_moment) * rotated
    o_m2[...] = decay_moment * m2[...] + (1.0 - decay_moment) * rotated * rotated
    o_l[...] = decay_factor * lf[...] + scale * left[...].astype(F32)
    o_r[...] = decay_factor * rf[...] + scale * right[...].astype(F32)
    o_u[...] = update[...]


def per_device(gradient, first_moment, second_moment, left_factor, right_factor, left_basis, right_basis):
    ins = [a.reshape(N, N) for a in (gradient, first_moment, second_moment, left_basis, right_basis)]
    block = pltpu.VMEM((N, N), BF)
    wide = pltpu.VMEM((N, N), F32)

    def many(n, dtype=BF, width=N):
        return pltpu.VMEM((n, N, width), dtype)

    sums = pl.pallas_call(
        kernel,
        name="soap",
        out_shape=[jax.ShapeDtypeStruct((N, N), BF)] * 4,
        in_specs=[pl.BlockSpec(memory_space=pltpu.HBM)] * 5,
        out_specs=[pl.BlockSpec(memory_space=pltpu.VMEM)] * 4,
        scratch_shapes=[block] * 3
        + [wide] * 2
        + [many(2)] * 2
        + [block] * 3
        + [many(16)] * 5
        + [block] * 12
        + [wide] * 3
        + [pltpu.VMEM((N, 128), BF)] * 2
        + ([many(16, F32, 128)] + [many(15, BF, 128)] * 2) * 2
        + [many(16, F32), many(15), many(15)]
        + ([many(8, F32, 128)] + [many(8, BF, 128)] * 2 + [many(7, BF, 128)] * 2) * 2
        + [many(8, F32), many(8), many(8), many(7), many(7)]
        + [pltpu.SemaphoreType.DMA((NSEND,)), pltpu.SemaphoreType.DMA((NRECV,))]
        + [pltpu.SemaphoreType.DMA((5,))],
        compiler_params=pltpu.CompilerParams(collective_id=0, has_side_effects=True, vmem_limit_bytes=LIMIT * 1024 * 1024),
    )(*ins)
    old = [a.reshape(N, N) for a in (first_moment, second_moment, left_factor, right_factor)]
    outs = pl.pallas_call(
        blend,
        name="blend",
        out_shape=[jax.ShapeDtypeStruct((N, N), F32)] * 4 + [jax.ShapeDtypeStruct((N, N), BF)],
        in_specs=[pl.BlockSpec(memory_space=pltpu.VMEM)] * 8,
        out_specs=[pl.BlockSpec(memory_space=pltpu.VMEM)] * 5,
        compiler_params=pltpu.CompilerParams(vmem_limit_bytes=LIMIT * 1024 * 1024),
    )(*sums, *old)
    return tuple(o.reshape(1, N, N) for o in outs)


def solution(mesh):
    spec = P(None, "mp", "dp")
    return jax.shard_map(
        per_device,
        mesh=mesh,
        in_specs=(spec,) * 5 + (P(None, "dp", "mp"), spec),
        out_specs=(spec,) * 5,
        check_vma=False,
    )
```

```python
import jax
import jax.numpy as jnp
from jax import lax
from jax.experimental import pallas as pl
from jax.experimental.pallas import tpu as pltpu
from jax.sharding import PartitionSpec as P

decay_moment = 0.95
decay_factor = 0.95
epsilon = 1e-08
N = 256
NZ = 8
NX = 4
NY = 4
NSEND = 25
NRECV = 139
LIMIT = 62

BF = jnp.bfloat16
F32 = jnp.float32
MESH = pl.DeviceIdType.MESH
TIMES = {
    "mi": (0,),
    "gz": (1, 2, 4, 6, 7, 10, 18, 11, 21, 17, 23, 19, 35, 29, 34, 31, 38, 41, 52, 39, 30, 53,),
    "hq": (3,),
    "qp": (5, 15, 24, 22, 28, 33, 45, 46, 48,),
    "hl": (8,),
    "gp": (9, 37, 47, 50, 67, 56, 63, 75, 65,),
    "lz": (12, 13, 14, 16, 32, 25, 27, 26, 40, 43, 44, 36, 61, 60, 59, 51, 64, 70, 68, 66, 57, 72,),
    "mm": (20,),
    "hm": (42,),
    "t": (49, 54,),
    "tp": (55, 58, 73, 62, 69, 71, 82, 78, 80,),
    "rp": (74, 111, 114, 121, 123, 129, 147, 159,),
    "ls": (76, 79, 93, 81, 102, 113, 87, 91, 86, 88, 94, 100, 99, 95, 104, 106, 107, 110, 117, 122, 115, 120, 139, 155, 143, 144,),
    "r": (77, 83, 84,),
    "b0": (85, 90, 96, 97, 103, 101, 112, 118,),
    "b1": (89, 92, 98, 105, 109, 108, 116, 128,),
    "u0": (119, 124, 142, 125, 133, 146, 126, 127, 131, 132, 141, 145, 153, 156, 162, 163,),
    "u1": (130, 134, 150, 135, 148, 154, 136, 138, 137, 140, 151, 152, 158, 160, 164, 165,),
    "rr": (149,),
    "rl": (157,),
    "rt": (161,),
}


def dot(a, b):
    return jnp.dot(a, b, preferred_element_type=F32)


def turned(a):
    return a.astype(F32).T


class Place:
    def __init__(self):
        j, i = lax.axis_index("dp"), lax.axis_index("mp")
        self.z, self.y = j // 2, (i // 8) * 2 + j % 2
        self.x, self.c = (i // 2) % NX, i % 2
        self.away = j % 2 != self.c

    def row(self, dy=0, dx=0):
        y = lax.rem(self.y + dy + NY, NY)
        return (y // 2) * 8 + lax.rem(self.x + dx + NX, NX) * 2 + y % 2

    def column(self, dz=0, dc=0):
        return lax.rem(self.z + dz + NZ, NZ) * 2 + (1 - self.c if dc else self.c)

    def device(self, dz=0, dy=0, dx=0, dc=0):
        y = lax.rem(self.y + dy + NY, NY)
        c = 1 - self.c if dc else self.c
        z, x = lax.rem(self.z + dz + NZ, NZ), lax.rem(self.x + dx + NX, NX)
        return {"dp": z * 2 + y % 2, "mp": (y // 2) * 8 + x * 2 + c}

    def twin(self):
        y = self.y + 1 - 2 * (self.y % 2)
        return {"dp": self.z * 2 + y % 2, "mp": (y // 2) * 8 + self.x * 2 + 1 - self.c}


class Wires:
    def __init__(self, send_sem, recv_sem):
        self.send_sem, self.recv_sem = send_sem, recv_sem
        self.sends = self.recvs = 0

    def flow(self, gauge):
        self.sends += 1
        assert self.sends <= NSEND
        return Flow(self, self.send_sem.at[self.sends - 1], gauge)

    def receiver(self):
        self.recvs += 1
        assert self.recvs <= NRECV
        return self.recv_sem.at[self.recvs - 1]


class Flow:
    def __init__(self, wires, send_sem, gauge):
        self.wires, self.send_sem, self.gauge = wires, send_sem, gauge
        self.groups = {}

    def send(self, group, src, dst, device):
        if group not in self.groups:
            self.groups[group] = self.wires.receiver()
        pltpu.make_async_remote_copy(
            src_ref=src,
            dst_ref=dst,
            send_sem=self.send_sem,
            recv_sem=self.groups[group],
            device_id=device,
            device_id_type=MESH,
        ).start()

    def pause(self, sem, quarters):
        if quarters >= 4:
            assert quarters % 4 == 0
            size = self.gauge.at[pl.ds(0, quarters // 4)]
        else:
            size = self.gauge.at[0, pl.ds(0, quarters * 64)]
        pltpu.make_async_copy(size, size, sem).wait()

    def wait(self, group, quarters):
        self.pause(self.groups[group], quarters)

    def drain(self):
        self.pause(self.send_sem, 60)


WAYS = (1, -1)


def half(f):
    return pl.ds(f * 128, 128)


def quarter(f, way):
    return pl.ds(f * 128 + (0 if way == 1 else 64), 64)


def part(h):
    return pl.ds(h * 64, 64)


def along(f, a=0, b=0):
    return {"dy": a, "dx": b} if f == 0 else {"dy": b, "dx": a}


def gather_z(w, p, own, buf, ready=lambda h: None):
    def start(h):
        def step():
            ready(h)
            for way in WAYS:
                w.send((1, h), own.at[part(h)], buf.at[p.column(), part(h)], p.device(dz=way))
            if h == 3:
                w.send("C near", own, buf.at[p.column()], p.device(dc=1))

        return step

    def arrive(n, h):
        last = WAYS[h // 2]

        def step():
            w.wait((n, h), 2 if n < 4 else 1)
            for way in WAYS if n < 4 else (last,):
                ref = buf.at[p.column(-n * way), part(h)]
                if n < 3 or (n == 3 and way == last):
                    w.send((n + 1, h), ref, ref, p.device(dz=way))
            for way in WAYS if n < 4 else (last,):
                ref = buf.at[p.column(-n * way), part(h)]
                w.send("C near" if n < 3 else "C far", ref, ref, p.device(dc=1))

        return step

    def near_siblings():
        w.wait("C near", 4 * 5)

    def far_siblings():
        w.wait("C far", 4 * 3)

    return [start(h) for h in range(4)] + [arrive(n, h) for n in (1, 2, 3, 4) for h in range(4)] + [near_siblings, far_siblings]


def gather_plane(w, p, own, buf):
    def send(group, f, ref, dst=None, **to):
        w.send(group, ref, ref if dst is None else dst, p.device(**along(f, **to)))

    def block(f, a, b, rows):
        return buf.at[p.row(**along(f, a, b)), rows]

    def start():
        for stage in ("a", "b"):
            for f in (0, 1):
                for way in WAYS:
                    dst = buf.at[p.row(), half(f)]
                    if stage == "a":
                        send("a1", f, own.at[half(f)], dst, a=way)
                    else:
                        send(("b", 0), f, own.at[half(f)], dst, b=way)

    def first():
        w.wait("a1", 8)
        for f in (0, 1):
            for way in WAYS:
                send("a2", f, block(f, -way, 0, quarter(f, way)), a=way)
        for f in (0, 1):
            for way in WAYS:
                for v in WAYS:
                    send(("b", 1), f, block(f, -way, 0, half(f)), b=v)

    def second(q):
        def step():
            w.wait(("b", q), 8 if q != 1 else 16)
            for r in (1, -1) if q == 1 else (q,):
                for f in (0, 1):
                    for v in WAYS:
                        send(("bb", q), f, block(f, r, -v, quarter(f, v)), b=v)

        return step

    def opposite():
        w.wait("a2", 4)
        for f in (0, 1):
            for v in WAYS:
                send(("b", 2), f, block(f, 2, 0, half(f)), b=v)

    def last(q):
        def step():
            w.wait(("bb", q), 4 if q != 1 else 8)

        return step

    return [start, first, second(0), opposite, second(1), second(2), last(0), last(1), last(2)]


def scatter_plane(w, p, term, done, bufs):
    base, out, into = bufs
    early = [(dy, dx) for dy in range(4) for dx in range(4) if dy == 2 or dx == 2]
    late = [(dy, dx) for dy in range(4) for dx in range(4) if dy != 2 and dx != 2]

    def terms(places):
        for dy, dx in places:
            base[dy * 4 + dx] = term(p.row(dy, dx))

    def held(f, a, b, rows):
        d = along(f, a, b)
        return base[(d["dy"] % 4) * 4 + d["dx"] % 4, rows]

    def send(group, f, slot, rows, **to):
        w.send(group, out.at[slot, rows], into.at[slot, rows], p.device(**along(f, **to)))

    def far():
        terms(early)
        for q in (2, 1, -1, 0):
            for f in (0, 1):
                out[q % 4, half(f)] = held(f, q, 2, half(f)).astype(BF)
        for q in (2, 1, -1, 0):
            for f in (0, 1):
                for v in WAYS:
                    send((2, abs(q)), f, q % 4, quarter(f, v), b=v)

    def rest():
        terms(late)

    def near(q):
        def step():
            w.wait((2, q), 4 if q != 1 else 8)
            for r in (1, -1) if q == 1 else (q,):
                for f in (0, 1):
                    for n, v in enumerate(WAYS):
                        slot, rows = 4 + (r % 4) * 2 + n, quarter(f, v)
                        out[slot, half(f)] = held(f, r, v, half(f)).astype(BF)
                        out[slot, rows] = (held(f, r, v, rows) + into[r % 4, rows].astype(F32)).astype(BF)
                        send((1, q), f, slot, half(f), b=v)

        return step

    def line(f, q, rows):
        total = held(f, q, 0, rows)
        for n, v in enumerate(WAYS):
            total = total + into[4 + (q % 4) * 2 + n, rows].astype(F32)
        return total

    def opposite():
        w.wait((1, 2), 8)
        for f in (0, 1):
            out[12, half(f)] = line(f, 2, half(f)).astype(BF)
            for way in WAYS:
                send("a2", f, 12, quarter(f, way), a=way)

    def beside():
        w.wait((1, 1), 16)
        w.wait("a2", 4)
        for f in (0, 1):
            for n, way in enumerate(WAYS):
                rows = quarter(f, way)
                out[13 + n, half(f)] = line(f, way, half(f)).astype(BF)
                out[13 + n, rows] = (line(f, way, rows) + into[12, rows].astype(F32)).astype(BF)
                send("a1", f, 13 + n, half(f), a=way)

    def finish():
        w.wait((1, 0), 8)
        w.wait("a1", 8)
        for f in (0, 1):
            total = line(f, 0, half(f))
            for n in (0, 1):
                total = total + into[13 + n, half(f)].astype(F32)
            done(f, total)

    return [far, rest, near(2), near(1), opposite, near(0), beside, finish]


def scatter_z(w, p, term, done, bufs, parts=2):
    base, mate_out, mate_in, out, into = bufs
    stages = ((4, 3, 5), (2, 6), (1, 7, 0))
    size = N // parts

    def rows(h):
        return pl.ds(h * size, size)

    def slot(n, way):
        return 0 if n == 4 else 1 + (n - 1) * 2 + (0 if way == 1 else 1)

    def start(k):
        def step():
            for dz in stages[k]:
                mate_out[dz] = term(p.column(dz, 1)).astype(BF)
            for dz in stages[k]:
                w.send(("C", k), mate_out.at[dz], mate_in.at[dz], p.device(dc=1))
            for dz in stages[k]:
                base[dz] = term(p.column(dz))

        return step

    def chip(k):
        def step():
            w.wait(("C", k), 4 * len(stages[k]))
            for dz in stages[k]:
                base[dz] = base[dz] + mate_in[dz].astype(F32)

        return step

    def push(n, h):
        last = WAYS[h // (parts // 2)]

        def step():
            if n < 3:
                w.wait((n + 1, h), 8 // parts)
            if n == 2:
                w.wait((4, h), 4 // parts)
            for way in WAYS if n < 4 else (last,):
                total = base[(n * way) % 8, rows(h)]
                if n < 3:
                    total = total + into[slot(n + 1, way), rows(h)].astype(F32)
                if n == 2 and way == last:
                    total = total + into[0, rows(h)].astype(F32)
                out[slot(n, way), rows(h)] = total.astype(BF)
                to = p.device(dz=2 * way if n == 4 else way)
                w.send((n, h), out.at[slot(n, way), rows(h)], into.at[slot(n, way), rows(h)], to)

        return step

    def finish(h):
        def step():
            w.wait((1, h), 8 // parts)
            total = base[0, rows(h)]
            for way in WAYS:
                total = total + into[slot(1, way), rows(h)].astype(F32)
            done(rows(h), total)

        return step

    steps = [start(0), start(1), start(2), chip(0), chip(1), chip(2)]
    return steps + [push(n, h) for n in (4, 3, 2, 1) for h in range(parts)] + [finish(h) for h in range(parts)]


def kernel(
    g_in, m1_in, m2_in, ql_in, qr_in,
    o_rot, o_l, o_r, o_u,
    g_0, ql_0, qr_0, m1_0, m2_0, mm_0, mm,
    g, ql, qr,
    gb, qlb, qrb, tb, gcb,
    g_turned, ql_turned, t_own, d_turned, u_0, u_1,
    left, left_1, right, right_1, rot_0, rot_1,
    acc_t, rot, right_sum,
    back_0, back_1,
    pb_0, po_0, pi_0, pb_1, po_1, pi_1, pb_r, po_r, pi_r,
    zb_0, zmo_0, zmi_0, zo_0, zi_0, zb_1, zmo_1, zmi_1, zo_1, zi_1, zb_l, zmo_l, zmi_l, zo_l, zi_l,
    send_sem, recv_sem, load_sem,
):
    p = Place()
    w = Wires(send_sem, recv_sem)
    home = jnp.logical_not(p.away)
    peers = [p.device(dz=1), p.device(dz=-1), p.device(dy=1), p.device(dy=-1), p.device(dx=1), p.device(dx=-1), p.device(dc=1), p.twin()]
    peers += [p.device(dz=2), p.device(dz=-2), p.device(dx=2), p.device(dy=2)]

    barrier = pltpu.get_barrier_semaphore()
    for peer in peers:
        pl.semaphore_signal(barrier, inc=1, device_id=peer, device_id_type=MESH)

    loads = {}
    for n, (name, src, dst) in enumerate((("g", g_in, g_0), ("qr", qr_in, qr_0), ("ql", ql_in, ql_0), ("m1", m1_in, m1_0), ("m2", m2_in, m2_0))):
        loads[name] = pltpu.make_async_copy(src, dst, load_sem.at[n])
        loads[name].start()
    loads["g"].wait()
    loads["qr"].wait()
    pl.semaphore_wait(barrier, len(peers))

    moves = {}

    def move(name, src, dst):
        copy = pltpu.make_async_remote_copy(
            src_ref=src,
            dst_ref=dst,
            send_sem=w.flow(None).send_sem,
            recv_sem=w.receiver(),
            device_id=p.twin(),
            device_id_type=MESH,
        )
        moves[name] = copy

        @pl.when(p.away)
        def _():
            copy.start()

        @pl.when(home)
        def _():
            dst[...] = src[...]

    def moved(name):
        @pl.when(p.away)
        def _():
            moves[name].wait_recv()

    def move_in():
        for h in range(4):
            move(("g", h), g_0.at[part(h)], g.at[part(h)])
        move("qr", qr_0, qr)
        loads["ql"].wait()
        move("ql", ql_0, ql)

    def have_qr():
        moved("qr")

    def have_ql():
        gb[p.column()] = g[...]
        gcb[p.row()] = g[...]
        qrb[p.row()] = qr[...]
        moved("ql")
        ql_turned[...] = turned(ql[...]).astype(BF)
        qlb[p.column()] = ql_turned[...]

    def move_moments():
        loads["m1"].wait()
        loads["m2"].wait()
        mm_0[0] = m1_0[...].astype(BF)
        mm_0[1] = m2_0[...].astype(BF)
        move("m", mm_0, mm)
        g_turned[...] = turned(g[...]).astype(BF)

    def have_moments():
        moved("m")

    def gathered(acc, lefts, rights, keys, fresh):
        total = None if fresh else acc[...]
        for k in keys:
            term = dot(lefts[k], rights[k])
            total = term if total is None else total + term
        acc[...] = total

    def product_t(dzs, fresh=False, last=False):
        def product():
            gathered(acc_t, gb, qrb, [p.column(dz, dc) for dz in dzs for dc in (0, 1)], fresh)
            if last:
                t_own[...] = acc_t[...].astype(BF)
                tb[p.row()] = t_own[...]

        return product

    def rotate(keys, fresh=False):
        def rotated():
            gathered(rot, qlb, tb, [p.row(dy, dx) for dy, dx in keys], fresh)

        return rotated

    def moments():
        rotated = rot[...]
        first = decay_moment * mm[0].astype(F32) + (1.0 - decay_moment) * rotated
        second = decay_moment * mm[1].astype(F32) + (1.0 - decay_moment) * rotated * rotated
        direction = (first / (jnp.sqrt(second) + epsilon)).astype(BF)
        d_turned[...] = turned(direction).astype(BF)

    def left_term(k):
        return lax.dot_general(g[...], gcb[k], (((1,), (1,)), ((), ())), preferred_element_type=F32)

    def left_done(h, total):
        left[h] = total.astype(BF)

    def right_done(f, total):
        right_sum[half(f)] = total

    def right_term(k):
        return dot(g_turned[...], gb[k])

    backs = (back_0, back_1)

    def back_term(n):
        return lambda k: dot(d_turned[...], qlb[k, :, half(n)])

    def back_done(n):
        def store(f, total):
            backs[n][half(f)] = total.astype(BF)

        return store

    def update_term(n):
        return lambda k: dot(qrb[k], backs[n][...])

    def update_done(n):
        def store(rows, total):
            u_0[half(n), rows] = total.T.astype(BF)
            move(("u", n, rows.start), u_0.at[half(n), rows], u_1.at[half(n), rows])

        return store

    def return_rotated():
        rot_0[...] = rot[...].astype(BF)
        move("rot", rot_0, rot_1)

    def return_right():
        right[...] = right_sum[...].T.astype(BF)
        move("right", right, right_1)

    def return_left():
        move("left", left, left_1)

    def results():
        for name in moves:
            if name in ("rot", "right", "left") or name[0] == "u":
                moved(name)
        for src, dst in ((rot_1, o_rot), (right_1, o_r), (left_1, o_l), (u_1, o_u)):
            dst[...] = src[...]

    near_rows = [(0, 0), (1, 0), (3, 0), (0, 1), (0, 3), (1, 1), (3, 1), (1, 3), (3, 3)]
    far_rows = [(2, 0), (0, 2), (2, 1), (2, 3), (1, 2), (3, 2), (2, 2)]
    gauge = {"gz": gb, "qp": qrb, "lz": qlb, "tp": tb, "b0": po_0, "b1": po_1, "u0": po_0, "u1": po_1, "gp": gcb, "ls": po_r, "rp": po_r}
    f = {name: w.flow(ref) for name, ref in gauge.items()}
    flows = {
        "mi": [move_in],
        "hq": [have_qr],
        "hl": [have_ql],
        "mm": [move_moments],
        "hm": [have_moments],
        "gz": gather_z(f["gz"], p, g, gb, lambda h: moved(("g", h))),
        "qp": gather_plane(f["qp"], p, qr, qrb),
        "lz": gather_z(f["lz"], p, ql_turned, qlb),
        "t": [product_t([0, 1, 7, 2, 6], fresh=True), product_t([3, 5, 4], last=True)],
        "tp": gather_plane(f["tp"], p, t_own, tb),
        "r": [rotate(near_rows, fresh=True), rotate(far_rows), moments],
        "b0": scatter_plane(f["b0"], p, back_term(0), back_done(0), (pb_0, po_0, pi_0)),
        "b1": scatter_plane(f["b1"], p, back_term(1), back_done(1), (pb_1, po_1, pi_1)),
        "u0": scatter_z(f["u0"], p, update_term(0), update_done(0), (zb_0, zmo_0, zmi_0, zo_0, zi_0)),
        "u1": scatter_z(f["u1"], p, update_term(1), update_done(1), (zb_1, zmo_1, zmi_1, zo_1, zi_1)),
        "gp": gather_plane(f["gp"], p, g, gcb),
        "ls": scatter_z(f["ls"], p, left_term, left_done, (zb_l, zmo_l, zmi_l, zo_l, zi_l), parts=4),
        "rp": scatter_plane(f["rp"], p, right_term, right_done, (pb_r, po_r, pi_r)),
        "rr": [return_rotated],
        "rl": [return_left],
        "rt": [return_right],
    }
    plan = [(t, step) for name, steps in flows.items() for t, step in zip(TIMES[name], steps, strict=True)]
    for _, step in sorted(plan, key=lambda item: item[0]):
        step()
    results()
    for flow in f.values():
        flow.drain()

    @pl.when(p.away)
    def _():
        for copy in moves.values():
            copy.wait_send()


def blend(rot, left, right, update, m1, m2, lf, rf, o_m1, o_m2, o_l, o_r, o_u):
    rotated = rot[...].astype(F32)
    scale = 1.0 - decay_factor
    o_m1[...] = decay_moment * m1[...] + (1.0 - decay_moment) * rotated
    o_m2[...] = decay_moment * m2[...] + (1.0 - decay_moment) * rotated * rotated
    o_l[...] = decay_factor * lf[...] + scale * left[...].astype(F32)
    o_r[...] = decay_factor * rf[...] + scale * right[...].astype(F32)
    o_u[...] = update[...]


def per_device(gradient, first_moment, second_moment, left_factor, right_factor, left_basis, right_basis):
    ins = [a.reshape(N, N) for a in (gradient, first_moment, second_moment, left_basis, right_basis)]
    block = pltpu.VMEM((N, N), BF)
    wide = pltpu.VMEM((N, N), F32)

    def many(n, dtype=BF, width=N):
        return pltpu.VMEM((n, N, width), dtype)

    sums = pl.pallas_call(
        kernel,
        name="soap",
        out_shape=[jax.ShapeDtypeStruct((N, N), BF)] * 4,
        in_specs=[pl.BlockSpec(memory_space=pltpu.HBM)] * 5,
        out_specs=[pl.BlockSpec(memory_space=pltpu.VMEM)] * 4,
        scratch_shapes=[block] * 3
        + [wide] * 2
        + [many(2)] * 2
        + [block] * 3
        + [many(16)] * 5
        + [block] * 12
        + [wide] * 3
        + [pltpu.VMEM((N, 128), BF)] * 2
        + ([many(16, F32, 128)] + [many(15, BF, 128)] * 2) * 2
        + [many(16, F32), many(15), many(15)]
        + ([many(8, F32, 128)] + [many(8, BF, 128)] * 2 + [many(7, BF, 128)] * 2) * 2
        + [many(8, F32), many(8), many(8), many(7), many(7)]
        + [pltpu.SemaphoreType.DMA((NSEND,)), pltpu.SemaphoreType.DMA((NRECV,))]
        + [pltpu.SemaphoreType.DMA((5,))],
        compiler_params=pltpu.CompilerParams(collective_id=0, has_side_effects=True, vmem_limit_bytes=LIMIT * 1024 * 1024),
    )(*ins)
    old = [a.reshape(N, N) for a in (first_moment, second_moment, left_factor, right_factor)]
    outs = pl.pallas_call(
        blend,
        name="blend",
        out_shape=[jax.ShapeDtypeStruct((N, N), F32)] * 4 + [jax.ShapeDtypeStruct((N, N), BF)],
        in_specs=[pl.BlockSpec(memory_space=pltpu.VMEM)] * 8,
        out_specs=[pl.BlockSpec(memory_space=pltpu.VMEM)] * 5,
        compiler_params=pltpu.CompilerParams(vmem_limit_bytes=LIMIT * 1024 * 1024),
    )(*sums, *old)
    return tuple(o.reshape(1, N, N) for o in outs)


def solution(mesh):
    spec = P(None, "mp", "dp")
    return jax.shard_map(
        per_device,
        mesh=mesh,
        in_specs=(spec,) * 5 + (P(None, "dp", "mp"), spec),
        out_specs=(spec,) * 5,
        check_vma=False,
    )
```

```python
import jax
import jax.numpy as jnp
from jax import lax
from jax.experimental import pallas as pl
from jax.experimental.pallas import tpu as pltpu
from jax.sharding import PartitionSpec as P

decay_moment = 0.95
decay_factor = 0.95
epsilon = 1e-08
N = 256
NZ = 8
NX = 4
NY = 4
NSEND = 25
NRECV = 139
LIMIT = 62

BF = jnp.bfloat16
F32 = jnp.float32
MESH = pl.DeviceIdType.MESH
TIMES = {
    "mi": (0,),
    "gz": (1, 2, 4, 6, 7, 10, 18, 11, 21, 17, 23, 19, 35, 29, 34, 31, 38, 41, 52, 39, 30, 53,),
    "hq": (3,),
    "qp": (5, 15, 24, 22, 28, 33, 45, 46, 48,),
    "hl": (8,),
    "gp": (9, 37, 47, 50, 67, 56, 63, 75, 65,),
    "lz": (12, 13, 14, 16, 32, 25, 27, 26, 40, 43, 44, 36, 61, 60, 59, 51, 64, 70, 68, 66, 57, 72,),
    "mm": (20,),
    "hm": (42,),
    "t": (49, 54,),
    "tp": (55, 58, 73, 62, 69, 71, 82, 78, 80,),
    "rp": (74, 111, 114, 121, 123, 129, 147, 159,),
    "ls": (76, 79, 93, 81, 102, 113, 87, 91, 86, 88, 94, 100, 99, 95, 104, 106, 107, 110, 117, 122, 115, 120, 139, 155, 143, 144,),
    "r": (77, 83, 84,),
    "b0": (85, 90, 96, 97, 103, 101, 112, 118,),
    "b1": (89, 92, 98, 105, 109, 108, 116, 128,),
    "u0": (119, 124, 142, 125, 133, 146, 126, 127, 131, 132, 141, 145, 153, 156, 162, 163,),
    "u1": (130, 134, 150, 135, 148, 154, 136, 138, 137, 140, 151, 152, 158, 160, 164, 165,),
    "rr": (149,),
    "rl": (157,),
    "rt": (161,),
}


def dot(a, b):
    return jnp.dot(a, b, preferred_element_type=F32)


def turned(a):
    return a.astype(F32).T


class Place:
    def __init__(self):
        j, i = lax.axis_index("dp"), lax.axis_index("mp")
        self.z, self.y = j // 2, (i // 8) * 2 + j % 2
        self.x, self.c = (i // 2) % NX, i % 2
        self.away = j % 2 != self.c

    def row(self, dy=0, dx=0):
        y = lax.rem(self.y + dy + NY, NY)
        return (y // 2) * 8 + lax.rem(self.x + dx + NX, NX) * 2 + y % 2

    def column(self, dz=0, dc=0):
        return lax.rem(self.z + dz + NZ, NZ) * 2 + (1 - self.c if dc else self.c)

    def device(self, dz=0, dy=0, dx=0, dc=0):
        y = lax.rem(self.y + dy + NY, NY)
        c = 1 - self.c if dc else self.c
        z, x = lax.rem(self.z + dz + NZ, NZ), lax.rem(self.x + dx + NX, NX)
        return {"dp": z * 2 + y % 2, "mp": (y // 2) * 8 + x * 2 + c}

    def twin(self):
        y = self.y + 1 - 2 * (self.y % 2)
        return {"dp": self.z * 2 + y % 2, "mp": (y // 2) * 8 + self.x * 2 + 1 - self.c}

    def final(self, dz):
        y = self.y + jnp.where(self.away, 1 - 2 * (self.y % 2), 0)
        c = jnp.where(self.away, 1 - self.c, self.c)
        return {"dp": lax.rem(self.z + dz + NZ, NZ) * 2 + y % 2, "mp": (y // 2) * 8 + self.x * 2 + c}


class Wires:
    def __init__(self, send_sem, recv_sem):
        self.send_sem, self.recv_sem = send_sem, recv_sem
        self.sends = self.recvs = 0

    def flow(self, gauge):
        self.sends += 1
        assert self.sends <= NSEND
        return Flow(self, self.send_sem.at[self.sends - 1], gauge)

    def receiver(self):
        self.recvs += 1
        assert self.recvs <= NRECV
        return self.recv_sem.at[self.recvs - 1]


class Flow:
    def __init__(self, wires, send_sem, gauge):
        self.wires, self.send_sem, self.gauge = wires, send_sem, gauge
        self.groups = {}

    def send(self, group, src, dst, device):
        if group not in self.groups:
            self.groups[group] = self.wires.receiver()
        pltpu.make_async_remote_copy(
            src_ref=src,
            dst_ref=dst,
            send_sem=self.send_sem,
            recv_sem=self.groups[group],
            device_id=device,
            device_id_type=MESH,
        ).start()

    def pause(self, sem, quarters):
        if quarters >= 4:
            assert quarters % 4 == 0
            size = self.gauge.at[pl.ds(0, quarters // 4)]
        else:
            size = self.gauge.at[0, pl.ds(0, quarters * 64)]
        pltpu.make_async_copy(size, size, sem).wait()

    def wait(self, group, quarters):
        self.pause(self.groups[group], quarters)

    def drain(self):
        self.pause(self.send_sem, 60)


WAYS = (1, -1)


def half(f):
    return pl.ds(f * 128, 128)


def quarter(f, way):
    return pl.ds(f * 128 + (0 if way == 1 else 64), 64)


def part(h):
    return pl.ds(h * 64, 64)


def along(f, a=0, b=0):
    return {"dy": a, "dx": b} if f == 0 else {"dy": b, "dx": a}


def gather_z(w, p, own, buf, ready=lambda h: None):
    def start(h):
        def step():
            ready(h)
            for way in WAYS:
                w.send((1, h), own.at[part(h)], buf.at[p.column(), part(h)], p.device(dz=way))
            if h == 3:
                w.send("C near", own, buf.at[p.column()], p.device(dc=1))

        return step

    def arrive(n, h):
        last = WAYS[h // 2]

        def step():
            w.wait((n, h), 2 if n < 4 else 1)
            for way in WAYS if n < 4 else (last,):
                ref = buf.at[p.column(-n * way), part(h)]
                if n < 3 or (n == 3 and way == last):
                    w.send((n + 1, h), ref, ref, p.device(dz=way))
            for way in WAYS if n < 4 else (last,):
                ref = buf.at[p.column(-n * way), part(h)]
                w.send("C near" if n < 3 else "C far", ref, ref, p.device(dc=1))

        return step

    def near_siblings():
        w.wait("C near", 4 * 5)

    def far_siblings():
        w.wait("C far", 4 * 3)

    return [start(h) for h in range(4)] + [arrive(n, h) for n in (1, 2, 3, 4) for h in range(4)] + [near_siblings, far_siblings]


def gather_plane(w, p, own, buf):
    def send(group, f, ref, dst=None, **to):
        w.send(group, ref, ref if dst is None else dst, p.device(**along(f, **to)))

    def block(f, a, b, rows):
        return buf.at[p.row(**along(f, a, b)), rows]

    def start():
        for stage in ("a", "b"):
            for f in (0, 1):
                for way in WAYS:
                    dst = buf.at[p.row(), half(f)]
                    if stage == "a":
                        send("a1", f, own.at[half(f)], dst, a=way)
                    else:
                        send(("b", 0), f, own.at[half(f)], dst, b=way)

    def first():
        w.wait("a1", 8)
        for f in (0, 1):
            for way in WAYS:
                send("a2", f, block(f, -way, 0, quarter(f, way)), a=way)
        for f in (0, 1):
            for way in WAYS:
                for v in WAYS:
                    send(("b", 1), f, block(f, -way, 0, half(f)), b=v)

    def second(q):
        def step():
            w.wait(("b", q), 8 if q != 1 else 16)
            for r in (1, -1) if q == 1 else (q,):
                for f in (0, 1):
                    for v in WAYS:
                        send(("bb", q), f, block(f, r, -v, quarter(f, v)), b=v)

        return step

    def opposite():
        w.wait("a2", 4)
        for f in (0, 1):
            for v in WAYS:
                send(("b", 2), f, block(f, 2, 0, half(f)), b=v)

    def last(q):
        def step():
            w.wait(("bb", q), 4 if q != 1 else 8)

        return step

    return [start, first, second(0), opposite, second(1), second(2), last(0), last(1), last(2)]


def scatter_plane(w, p, term, done, bufs):
    base, out, into = bufs
    early = [(dy, dx) for dy in range(4) for dx in range(4) if dy == 2 or dx == 2]
    late = [(dy, dx) for dy in range(4) for dx in range(4) if dy != 2 and dx != 2]

    def terms(places):
        for dy, dx in places:
            base[dy * 4 + dx] = term(p.row(dy, dx))

    def held(f, a, b, rows):
        d = along(f, a, b)
        return base[(d["dy"] % 4) * 4 + d["dx"] % 4, rows]

    def send(group, f, slot, rows, **to):
        w.send(group, out.at[slot, rows], into.at[slot, rows], p.device(**along(f, **to)))

    def far():
        terms(early)
        for q in (2, 1, -1, 0):
            for f in (0, 1):
                out[q % 4, half(f)] = held(f, q, 2, half(f)).astype(BF)
        for q in (2, 1, -1, 0):
            for f in (0, 1):
                for v in WAYS:
                    send((2, abs(q)), f, q % 4, quarter(f, v), b=v)

    def rest():
        terms(late)

    def near(q):
        def step():
            w.wait((2, q), 4 if q != 1 else 8)
            for r in (1, -1) if q == 1 else (q,):
                for f in (0, 1):
                    for n, v in enumerate(WAYS):
                        slot, rows = 4 + (r % 4) * 2 + n, quarter(f, v)
                        out[slot, half(f)] = held(f, r, v, half(f)).astype(BF)
                        out[slot, rows] = (held(f, r, v, rows) + into[r % 4, rows].astype(F32)).astype(BF)
                        send((1, q), f, slot, half(f), b=v)

        return step

    def line(f, q, rows):
        total = held(f, q, 0, rows)
        for n, v in enumerate(WAYS):
            total = total + into[4 + (q % 4) * 2 + n, rows].astype(F32)
        return total

    def opposite():
        w.wait((1, 2), 8)
        for f in (0, 1):
            out[12, half(f)] = line(f, 2, half(f)).astype(BF)
            for way in WAYS:
                send("a2", f, 12, quarter(f, way), a=way)

    def beside():
        w.wait((1, 1), 16)
        w.wait("a2", 4)
        for f in (0, 1):
            for n, way in enumerate(WAYS):
                rows = quarter(f, way)
                out[13 + n, half(f)] = line(f, way, half(f)).astype(BF)
                out[13 + n, rows] = (line(f, way, rows) + into[12, rows].astype(F32)).astype(BF)
                send("a1", f, 13 + n, half(f), a=way)

    def finish():
        w.wait((1, 0), 8)
        w.wait("a1", 8)
        for f in (0, 1):
            total = line(f, 0, half(f))
            for n in (0, 1):
                total = total + into[13 + n, half(f)].astype(F32)
            done(f, total)

    return [far, rest, near(2), near(1), opposite, near(0), beside, finish]


def scatter_z(w, p, term, done, bufs, parts=2, move=None, moved=None):
    base, mate_out, mate_in, out, into = bufs
    stages = ((4, 3, 5), (2, 6), (1, 7, 0))
    size = N // parts

    def rows(h):
        return pl.ds(h * size, size)

    def slot(n, way):
        return 0 if n == 4 else 1 + (n - 1) * 2 + (0 if way == 1 else 1)

    def start(k):
        def step():
            for dz in stages[k]:
                mate_out[dz] = term(p.column(dz, 1)).astype(BF)
            for dz in stages[k]:
                w.send(("C", k), mate_out.at[dz], mate_in.at[dz], p.device(dc=1))
            for dz in stages[k]:
                base[dz] = term(p.column(dz))

        return step

    def chip(k):
        def step():
            w.wait(("C", k), 4 * len(stages[k]))
            for dz in stages[k]:
                base[dz] = base[dz] + mate_in[dz].astype(F32)
            if k == 2 and move:
                out[7] = base[0].astype(BF)
                for h in range(parts):
                    move(h, out.at[7, rows(h)], into.at[7, rows(h)])

        return step

    def push(n, h):
        last = WAYS[h // (parts // 2)]

        def step():
            if n < 3:
                w.wait((n + 1, h), 8 // parts)
            if n == 2:
                w.wait((4, h), 4 // parts)
            for way in WAYS if n < 4 else (last,):
                total = base[(n * way) % 8, rows(h)]
                if n < 3:
                    total = total + into[slot(n + 1, way), rows(h)].astype(F32)
                if n == 2 and way == last:
                    total = total + into[0, rows(h)].astype(F32)
                out[slot(n, way), rows(h)] = total.astype(BF)
                to = p.final(way) if n == 1 and move else p.device(dz=2 * way if n == 4 else way)
                w.send((n, h), out.at[slot(n, way), rows(h)], into.at[slot(n, way), rows(h)], to)

        return step

    def finish(h):
        def step():
            w.wait((1, h), 8 // parts)
            if move:
                moved(h)
                total = into[7, rows(h)].astype(F32)
            else:
                total = base[0, rows(h)]
            for way in WAYS:
                total = total + into[slot(1, way), rows(h)].astype(F32)
            done(rows(h), total)

        return step

    steps = [start(0), start(1), start(2), chip(0), chip(1), chip(2)]
    return steps + [push(n, h) for n in (4, 3, 2, 1) for h in range(parts)] + [finish(h) for h in range(parts)]


def kernel(
    g_in, m1_in, m2_in, ql_in, qr_in,
    o_rot, o_l, o_r, o_u,
    g_0, ql_0, qr_0, m1_0, m2_0, mm_0, mm,
    g, ql, qr,
    gb, qlb, qrb, tb, gcb,
    g_turned, ql_turned, t_own, d_turned,
    left, left_1, right, right_1, rot_0, rot_1,
    acc_t, rot, right_sum,
    back_0, back_1,
    pb_0, po_0, pi_0, pb_1, po_1, pi_1, pb_r, po_r, pi_r,
    zb_0, zmo_0, zmi_0, zo_0, zi_0, zb_1, zmo_1, zmi_1, zo_1, zi_1, zb_l, zmo_l, zmi_l, zo_l, zi_l,
    send_sem, recv_sem, load_sem,
):
    p = Place()
    w = Wires(send_sem, recv_sem)
    home = jnp.logical_not(p.away)
    peers = [p.device(dz=1), p.device(dz=-1), p.device(dy=1), p.device(dy=-1), p.device(dx=1), p.device(dx=-1), p.device(dc=1), p.twin()]
    peers += [p.final(1), p.final(-1), p.device(dz=2), p.device(dz=-2), p.device(dx=2), p.device(dy=2)]

    barrier = pltpu.get_barrier_semaphore()
    for peer in peers:
        pl.semaphore_signal(barrier, inc=1, device_id=peer, device_id_type=MESH)

    loads = {}
    for n, (name, src, dst) in enumerate((("g", g_in, g_0), ("qr", qr_in, qr_0), ("ql", ql_in, ql_0), ("m1", m1_in, m1_0), ("m2", m2_in, m2_0))):
        loads[name] = pltpu.make_async_copy(src, dst, load_sem.at[n])
        loads[name].start()
    loads["g"].wait()
    loads["qr"].wait()
    pl.semaphore_wait(barrier, len(peers))

    moves = {}

    def move(name, src, dst):
        copy = pltpu.make_async_remote_copy(
            src_ref=src,
            dst_ref=dst,
            send_sem=w.flow(None).send_sem,
            recv_sem=w.receiver(),
            device_id=p.twin(),
            device_id_type=MESH,
        )
        moves[name] = copy

        @pl.when(p.away)
        def _():
            copy.start()

        @pl.when(home)
        def _():
            dst[...] = src[...]

    def moved(name):
        @pl.when(p.away)
        def _():
            moves[name].wait_recv()

    def move_in():
        for h in range(4):
            move(("g", h), g_0.at[part(h)], g.at[part(h)])
        move("qr", qr_0, qr)
        loads["ql"].wait()
        move("ql", ql_0, ql)

    def have_qr():
        moved("qr")

    def have_ql():
        gb[p.column()] = g[...]
        gcb[p.row()] = g[...]
        qrb[p.row()] = qr[...]
        moved("ql")
        ql_turned[...] = turned(ql[...]).astype(BF)
        qlb[p.column()] = ql_turned[...]

    def move_moments():
        loads["m1"].wait()
        loads["m2"].wait()
        mm_0[0] = m1_0[...].astype(BF)
        mm_0[1] = m2_0[...].astype(BF)
        move("m", mm_0, mm)
        g_turned[...] = turned(g[...]).astype(BF)

    def have_moments():
        moved("m")

    def gathered(acc, lefts, rights, keys, fresh):
        total = None if fresh else acc[...]
        for k in keys:
            term = dot(lefts[k], rights[k])
            total = term if total is None else total + term
        acc[...] = total

    def product_t(dzs, fresh=False, last=False):
        def product():
            gathered(acc_t, gb, qrb, [p.column(dz, dc) for dz in dzs for dc in (0, 1)], fresh)
            if last:
                t_own[...] = acc_t[...].astype(BF)
                tb[p.row()] = t_own[...]

        return product

    def rotate(keys, fresh=False):
        def rotated():
            gathered(rot, qlb, tb, [p.row(dy, dx) for dy, dx in keys], fresh)

        return rotated

    def moments():
        rotated = rot[...]
        first = decay_moment * mm[0].astype(F32) + (1.0 - decay_moment) * rotated
        second = decay_moment * mm[1].astype(F32) + (1.0 - decay_moment) * rotated * rotated
        direction = (first / (jnp.sqrt(second) + epsilon)).astype(BF)
        d_turned[...] = turned(direction).astype(BF)

    def left_term(k):
        return lax.dot_general(g[...], gcb[k], (((1,), (1,)), ((), ())), preferred_element_type=F32)

    def left_done(h, total):
        left[h] = total.astype(BF)

    def right_done(f, total):
        right_sum[half(f)] = total

    def right_term(k):
        return dot(g_turned[...], gb[k])

    backs = (back_0, back_1)

    def back_term(n):
        return lambda k: dot(d_turned[...], qlb[k, :, half(n)])

    def back_done(n):
        def store(f, total):
            backs[n][half(f)] = total.astype(BF)

        return store

    def update_term(n):
        return lambda k: dot(qrb[k], backs[n][...])

    def update_done(n):
        def store(rows, total):
            o_u[half(n), rows] = total.T.astype(BF)

        return store

    def piece(n):
        return lambda h, src, dst: move(("u", n, h), src, dst)

    def return_rotated():
        rot_0[...] = rot[...].astype(BF)
        move("rot", rot_0, rot_1)

    def return_right():
        right[...] = right_sum[...].T.astype(BF)
        move("right", right, right_1)

    def return_left():
        move("left", left, left_1)

    def results():
        for name in moves:
            if name in ("rot", "right", "left"):
                moved(name)
        for src, dst in ((rot_1, o_rot), (right_1, o_r), (left_1, o_l)):
            dst[...] = src[...]

    near_rows = [(0, 0), (1, 0), (3, 0), (0, 1), (0, 3), (1, 1), (3, 1), (1, 3), (3, 3)]
    far_rows = [(2, 0), (0, 2), (2, 1), (2, 3), (1, 2), (3, 2), (2, 2)]
    gauge = {"gz": gb, "qp": qrb, "lz": qlb, "tp": tb, "b0": po_0, "b1": po_1, "u0": po_0, "u1": po_1, "gp": gcb, "ls": po_r, "rp": po_r}
    f = {name: w.flow(ref) for name, ref in gauge.items()}
    flows = {
        "mi": [move_in],
        "hq": [have_qr],
        "hl": [have_ql],
        "mm": [move_moments],
        "hm": [have_moments],
        "gz": gather_z(f["gz"], p, g, gb, lambda h: moved(("g", h))),
        "qp": gather_plane(f["qp"], p, qr, qrb),
        "lz": gather_z(f["lz"], p, ql_turned, qlb),
        "t": [product_t([0, 1, 7, 2, 6], fresh=True), product_t([3, 5, 4], last=True)],
        "tp": gather_plane(f["tp"], p, t_own, tb),
        "r": [rotate(near_rows, fresh=True), rotate(far_rows), moments],
        "b0": scatter_plane(f["b0"], p, back_term(0), back_done(0), (pb_0, po_0, pi_0)),
        "b1": scatter_plane(f["b1"], p, back_term(1), back_done(1), (pb_1, po_1, pi_1)),
        "u0": scatter_z(f["u0"], p, update_term(0), update_done(0), (zb_0, zmo_0, zmi_0, zo_0, zi_0), move=piece(0), moved=lambda h: moved(("u", 0, h))),
        "u1": scatter_z(f["u1"], p, update_term(1), update_done(1), (zb_1, zmo_1, zmi_1, zo_1, zi_1), move=piece(1), moved=lambda h: moved(("u", 1, h))),
        "gp": gather_plane(f["gp"], p, g, gcb),
        "ls": scatter_z(f["ls"], p, left_term, left_done, (zb_l, zmo_l, zmi_l, zo_l, zi_l), parts=4),
        "rp": scatter_plane(f["rp"], p, right_term, right_done, (pb_r, po_r, pi_r)),
        "rr": [return_rotated],
        "rl": [return_left],
        "rt": [return_right],
    }
    plan = [(t, step) for name, steps in flows.items() for t, step in zip(TIMES[name], steps, strict=True)]
    for _, step in sorted(plan, key=lambda item: item[0]):
        step()
    results()
    for flow in f.values():
        flow.drain()

    @pl.when(p.away)
    def _():
        for copy in moves.values():
            copy.wait_send()


def blend(rot, left, right, update, m1, m2, lf, rf, o_m1, o_m2, o_l, o_r, o_u):
    rotated = rot[...].astype(F32)
    scale = 1.0 - decay_factor
    o_m1[...] = decay_moment * m1[...] + (1.0 - decay_moment) * rotated
    o_m2[...] = decay_moment * m2[...] + (1.0 - decay_moment) * rotated * rotated
    o_l[...] = decay_factor * lf[...] + scale * left[...].astype(F32)
    o_r[...] = decay_factor * rf[...] + scale * right[...].astype(F32)
    o_u[...] = update[...]


def per_device(gradient, first_moment, second_moment, left_factor, right_factor, left_basis, right_basis):
    ins = [a.reshape(N, N) for a in (gradient, first_moment, second_moment, left_basis, right_basis)]
    block = pltpu.VMEM((N, N), BF)
    wide = pltpu.VMEM((N, N), F32)

    def many(n, dtype=BF, width=N):
        return pltpu.VMEM((n, N, width), dtype)

    sums = pl.pallas_call(
        kernel,
        name="soap",
        out_shape=[jax.ShapeDtypeStruct((N, N), BF)] * 4,
        in_specs=[pl.BlockSpec(memory_space=pltpu.HBM)] * 5,
        out_specs=[pl.BlockSpec(memory_space=pltpu.VMEM)] * 4,
        scratch_shapes=[block] * 3
        + [wide] * 2
        + [many(2)] * 2
        + [block] * 3
        + [many(16)] * 5
        + [block] * 10
        + [wide] * 3
        + [pltpu.VMEM((N, 128), BF)] * 2
        + ([many(16, F32, 128)] + [many(15, BF, 128)] * 2) * 2
        + [many(16, F32), many(15), many(15)]
        + ([many(8, F32, 128)] + [many(8, BF, 128)] * 4) * 2
        + [many(8, F32), many(8), many(8), many(7), many(7)]
        + [pltpu.SemaphoreType.DMA((NSEND,)), pltpu.SemaphoreType.DMA((NRECV,))]
        + [pltpu.SemaphoreType.DMA((5,))],
        compiler_params=pltpu.CompilerParams(collective_id=0, has_side_effects=True, vmem_limit_bytes=LIMIT * 1024 * 1024),
    )(*ins)
    old = [a.reshape(N, N) for a in (first_moment, second_moment, left_factor, right_factor)]
    outs = pl.pallas_call(
        blend,
        name="blend",
        out_shape=[jax.ShapeDtypeStruct((N, N), F32)] * 4 + [jax.ShapeDtypeStruct((N, N), BF)],
        in_specs=[pl.BlockSpec(memory_space=pltpu.VMEM)] * 8,
        out_specs=[pl.BlockSpec(memory_space=pltpu.VMEM)] * 5,
        compiler_params=pltpu.CompilerParams(vmem_limit_bytes=LIMIT * 1024 * 1024),
    )(*sums, *old)
    return tuple(o.reshape(1, N, N) for o in outs)


def solution(mesh):
    spec = P(None, "mp", "dp")
    return jax.shard_map(
        per_device,
        mesh=mesh,
        in_specs=(spec,) * 5 + (P(None, "dp", "mp"), spec),
        out_specs=(spec,) * 5,
        check_vma=False,
    )
```
